128 devices in a mesh: dp: 32 (over z, x, core), tensor: 4 (over y).
Axes of the slice: x: 4, y: 4, z: 4, core: 2. Of those that a mesh axis runs over, the one named last changes fastest.
Arguments:
- activations: bfloat16 [64, 128, 4096], P('dp'), may hold values from -6 to 6
- out_grads: bfloat16 [64, 128, 20480], P('dp', None, 'tensor'), may hold values from -0.625 to 0.625
- act_scale: bfloat16 [64, 32], P('dp'), may hold values from 1 to 16
- grad_scale: bfloat16 [64, 1, 20480], P('dp', None, 'tensor'), may hold values from 1 to 72
- moment: float32 [20480, 4096], P(('tensor', 'dp')), may hold values from -0.6 to 0.6
- second: float32 [20480, 4096], P(('tensor', 'dp')), may hold values from 0.1 to 1
- master: float32 [20480, 4096], P(('tensor', 'dp')), may hold values from -0.0625 to 0.0625
Outputs:
- new_moment: float32 [20480, 4096], P(('tensor', 'dp'))
- new_second: float32 [20480, 4096], P(('tensor', 'dp'))
- new_master: float32 [20480, 4096], P(('tensor', 'dp'))
- weights: bfloat16 [20480, 4096], P(('tensor', 'dp'))
The draws below stay inside these ranges and needn't reach their ends.
All inputs are finite; a program needn't handle non-finite values.
Results may differ from the reference program's by a relative error of at most 0.015.
Values may be sent and summed in bfloat16 or wider, within the bound.
No kernel may reach another device: no remote copies, remote signals or barrier semaphores. Data moves between devices by JAX's collectives and lax.ppermute only.
A program may use at most 192 MiB of HBM per device.

```python
import math
import jax
import jax.numpy as jnp
from jax import lax

FF = 20480
ROWS = 4096
TILE = 128
TOK_DEV = 256
TOKENS = 8192
BLOCKS = 64
N_DP = 32


def draw_act_scale(key, part):
    upper = math.log(10.0)
    values = jnp.exp(jax.random.uniform(key, (BLOCKS, ROWS // TILE), jnp.float32, 0.0, upper))
    return values.astype(jnp.bfloat16)


def draw_grad_scale(key, part):
    upper = math.log(4.0)
    columns = jnp.arange(FF, dtype=jnp.float32) / (FF - 1)
    riser = jnp.exp(columns * math.log(9.0))
    base = jnp.exp(jax.random.uniform(key, (BLOCKS, 1, FF), jnp.float32, 0.0, upper))
    return (base * riser[None, None, :]).astype(jnp.bfloat16)


def with_spikes(values, rng, source, target, parts, factor):
    owner, partner = [(jnp.arange(values.shape[axis_at]) // (values.shape[axis_at] // parts)).reshape([-1 if axis == axis_at else 1 for axis in range(values.ndim)]) for axis_at in (source, target)]
    chosen = jax.random.permutation(rng, parts)[partner]
    strong = (owner == chosen) | (owner == (partner + parts // 2) % parts)
    return jnp.where(strong, factor * values, values)


def steps_of(key, extent, split, least, largest):
    gain, own = 1.0, jax.random.fold_in(key, 6)
    for dim, blocks in split:
        draws = jnp.exp(jax.random.uniform(jax.random.fold_in(own, dim), (blocks,), jnp.float32, least / len(split), largest / len(split)))
        gain = gain * jnp.repeat(draws, extent[dim] // blocks).reshape([-1 if axis == dim else 1 for axis in range(len(extent))])
    return gain


def scatter_about(rng, extent, scale, most, pieces=(), held_as=jnp.bfloat16):
    level = steps_of(rng, extent, pieces, -0.22, 0.18) if pieces else 1.0
    drawn = jax.random.normal(rng, extent, jnp.float32) * scale * level
    return jnp.minimum(jnp.maximum(drawn, -most), most).astype(held_as)


def gaussian_with(key, shape, deviation, reach, pieces, heavy, kind=jnp.bfloat16):
    entries = deviation * jax.random.normal(key, shape, jnp.float32)
    if pieces:
        entries = entries * steps_of(key, shape, pieces, -0.22, 0.18)
    return jnp.clip(with_spikes(entries, jax.random.fold_in(key, 3), *heavy), -reach, reach).astype(kind)


def setup_inputs(seed: int = 0) -> dict:
    streams_of = jax.random.split(jax.random.key(seed), 8)
    activations = scatter_about(streams_of[0], (BLOCKS, TILE, ROWS), 1.0, 6.0, ((0, 32),))
    out_grads = gaussian_with(streams_of[1], (BLOCKS, TILE, FF), (2.0 / TOKENS ** 0.5), 0.625, ((0, 32), (2, 4)), (0, 2, 32, 2.75))
    act_scale = draw_act_scale(jax.random.fold_in(streams_of[7], 71), 0)
    grad_scale = draw_grad_scale(jax.random.fold_in(streams_of[7], 71), 0)
    moment = scatter_about(streams_of[4], (FF, ROWS), 0.1, 0.6, ((0, 128),), jnp.float32)
    second = jnp.clip(jnp.exp(math.log(1.0) - 2.3025851 * jax.random.uniform(streams_of[5], (FF, ROWS), jnp.float32) ** steps_of(streams_of[5], (FF, ROWS), ((0, 128),), -0.2, 0.2)), 0.1, 1.0)
    master = scatter_about(streams_of[6], (FF, ROWS), 8192 ** -0.5, 0.0625, ((0, 128),), jnp.float32)
    return dict(activations=activations, out_grads=out_grads, act_scale=act_scale, grad_scale=grad_scale, moment=moment, second=second, master=master)


clip_rms = 1.0
beta_first = 0.9
beta_second = 0.95
learn_rate = 0.003
adam_eps = 1e-08

def widen(act_scale):
    tiles = act_scale.astype(jnp.float32)
    spread = jnp.broadcast_to(tiles[:, :, None], tiles.shape + (TILE,))
    return spread.reshape(tiles.shape[0], tiles.shape[1] * TILE)

def reference(activations, out_grads, act_scale, grad_scale, moment, second, master):
    acts_deq = (activations.astype(jnp.float32) * widen(act_scale)[:, None, :]).astype(jnp.bfloat16).reshape(TOKENS, ROWS)
    grads_deq = (out_grads.astype(jnp.float32) * grad_scale.astype(jnp.float32)).astype(jnp.bfloat16).reshape(TOKENS, FF)

    def add_group(group, total):
        start = (group * TOK_DEV).astype(jnp.int32)
        grads_group = lax.dynamic_slice_in_dim(grads_deq, start, TOK_DEV, 0)
        acts_group = lax.dynamic_slice_in_dim(acts_deq, start, TOK_DEV, 0)
        term = jnp.dot(grads_group.T, acts_group, preferred_element_type=jnp.float32)
        rounded = lax.optimization_barrier(term.astype(jnp.bfloat16))
        return total + rounded.astype(jnp.float32)
    grad = lax.fori_loop(0, N_DP, add_group, jnp.zeros((FF, ROWS), jnp.float32))
    norm = jnp.sqrt(jnp.sum(grad * grad))
    factor = jnp.minimum(1.0, clip_rms * jnp.sqrt(jnp.float32(FF * ROWS)) / norm)
    clipped = factor * grad
    new_moment = beta_first * moment + (1.0 - beta_first) * clipped
    new_second = beta_second * second + (1.0 - beta_second) * clipped * clipped
    new_master = master - learn_rate * new_moment / (jnp.sqrt(new_second) + adam_eps)
    weights = new_master.astype(jnp.bfloat16)
    return (new_moment, new_second, new_master, weights)
```

```python
import functools

import jax
import jax.numpy as jnp
from jax import lax
from jax.experimental import pallas as pl
from jax.experimental.pallas import tpu as pltpu
from jax.sharding import Mesh
from jax.sharding import PartitionSpec as P

FF = 20480
ROWS = 4096
TILE = 128
DP = ("z", "x", "c")
ALL = ("z", "x", "c", "y")
TENSOR_DP = ("y", "z", "x", "c")


clip_rms = 1.0
beta_first = 0.9
beta_second = 0.95
learn_rate = 0.003
adam_eps = 1e-08

VMEM = pltpu.VMEM


def ring(shift):
    return [(i, (i + shift) % 4) for i in range(4)]


SWAP = [(0, 1), (1, 0)]


def widen(act_scale):
    tiles = act_scale.astype(jnp.float32)
    spread = jnp.broadcast_to(tiles[:, :, None], tiles.shape + (TILE,))
    return spread.reshape(tiles.shape[0], tiles.shape[1] * TILE)


def prep_kernel(core_ref, grads_ref, scale_ref, keep_ref, send_ref, turned):
    tokens = grads_ref.shape[0] * grads_ref.shape[1]
    columns = grads_ref.shape[2]
    deq = (grads_ref[...].astype(jnp.float32) * scale_ref[...].astype(jnp.float32)).reshape(tokens, columns)
    turned[...] = deq.T.astype(jnp.bfloat16)
    own = columns // 8
    core = core_ref[0]
    for x in range(4):
        at = pl.multiple_of((2 * x + core) * own, 32)
        other = pl.multiple_of((2 * x + 1 - core) * own, 32)
        keep_ref[0, pl.ds(x * own, own), :] = turned[pl.ds(at, own), :]
        send_ref[0, pl.ds(x * own, own), :] = turned[pl.ds(other, own), :]


def prep_grads(core, out_grads, grad_scale):
    blocks, tile, columns = out_grads.shape
    tokens = blocks * tile
    part = columns // 4
    half = part // 2
    shape = jax.ShapeDtypeStruct((4, half, tokens), jnp.bfloat16)
    return pl.pallas_call(
        prep_kernel,
        grid_spec=pltpu.PrefetchScalarGridSpec(
            num_scalar_prefetch=1,
            grid=(4,),
            in_specs=[
                pl.BlockSpec((blocks, tile, part), lambda j, c: (0, 0, j)),
                pl.BlockSpec((blocks, 1, part), lambda j, c: (0, 0, j)),
            ],
            out_specs=[pl.BlockSpec((1, half, tokens), lambda j, c: (j, 0, 0))] * 2,
            scratch_shapes=[VMEM((part, tokens), jnp.bfloat16)],
        ),
        out_shape=[shape, shape],
        compiler_params=pltpu.CompilerParams(vmem_limit_bytes=24 * 2**20),
        cost_estimate=pl.CostEstimate(flops=10**9, bytes_accessed=4 * columns * tokens, transcendentals=0),
        name="prep",
    )(core, out_grads, grad_scale)


def product_kernel(terms, lefts, index_ref, *refs):
    x = index_ref[1]
    left_refs = refs[:lefts]
    right_refs = refs[lefts : lefts + len(terms)]
    outs = refs[lefts + len(terms) : lefts + len(terms) + 4]
    total = refs[-1]
    value = None
    for (left, side, start, size), right in zip(terms, right_refs):
        rows = left_refs[left][side, :, start : start + size]
        cols = right[...].reshape(size, right.shape[-1])
        term = jnp.dot(rows, cols, preferred_element_type=jnp.float32)
        value = term if value is None else value + term
    total[...] = value
    own = total.shape[0] // 4
    for k in range(4):
        at = pl.multiple_of(lax.rem(x + k, 4) * own, 32)
        outs[k][...] = total[pl.ds(at, own), :].astype(jnp.bfloat16)


WIDE = 256


def product(index, lefts, rights, width):
    left_specs = [pl.BlockSpec(a.shape, lambda j, i: (0, 0, 0)) for a in lefts]
    steps = width // WIDE
    terms, specs, arrays = [], [], []
    for left, side, start, size, array, lead in rights:
        terms.append((left, side, start, size))
        arrays.append(array)
        if lead is None:
            specs.append(pl.BlockSpec((size, WIDE), lambda j, i: (0, i[0] * steps + j)))
        elif array.ndim == 2:
            specs.append(pl.BlockSpec((size, WIDE), lambda j, i: (0, j)))
        else:
            specs.append(pl.BlockSpec((1, size, WIDE), lambda j, i, lead=lead: (lead, 0, j)))
    rows = lefts[0].shape[1]
    own = rows // 4
    depth = sum(t[3] for t in terms)
    return pl.pallas_call(
        functools.partial(product_kernel, terms, len(lefts)),
        grid_spec=pltpu.PrefetchScalarGridSpec(
            num_scalar_prefetch=1,
            grid=(steps,),
            in_specs=left_specs + specs,
            out_specs=[pl.BlockSpec((own, WIDE), lambda j, i: (0, j))] * 4,
            scratch_shapes=[VMEM((rows, WIDE), jnp.float32)],
        ),
        out_shape=[jax.ShapeDtypeStruct((own, width), jnp.bfloat16)] * 4,
        compiler_params=pltpu.CompilerParams(vmem_limit_bytes=28 * 2**20),
        cost_estimate=pl.CostEstimate(
            flops=2 * rows * depth * width, bytes_accessed=2 * depth * (rows + width), transcendentals=0
        ),
        name="product",
    )(index, *lefts, *arrays)


def per_device(activations, out_grads, act_scale, grad_scale, moment, second, master):
    z, x, c, y = (lax.axis_index(a).astype(jnp.int32) for a in ("z", "x", "c", "y"))
    rows = activations.shape[2]
    quarter = rows // 4
    tokens = activations.shape[0] * activations.shape[1]
    half = tokens // 2

    acts = (
        (activations.astype(jnp.float32) * widen(act_scale)[:, None, :]).astype(jnp.bfloat16).reshape(tokens, rows)
    )
    slab = lax.dynamic_slice_in_dim(acts, y * quarter, quarter, 1)

    def swap(a):
        return lax.ppermute(a, "c", SWAP)

    def along(axis, a, k):
        return lax.ppermute(a, axis, ring(k))

    from_z = {k: along("z", slab, k) for k in (1, 3, 2)}
    acts_other = swap(acts)

    keep, send = prep_grads(c[None], out_grads, grad_scale)
    pair = jnp.stack([keep, swap(send)], 1)
    left = [lax.dynamic_index_in_dim(pair, lax.rem(z + k, 4), 0, keepdims=False) for k in range(4)]
    left = [left[0]] + [along("z", left[k], k) for k in (1, 2, 3)]

    near = jnp.stack([from_z[1], from_z[3]])
    far = from_z[2]
    up_near, down_near = along("y", near, 1), along("y", near, 3)
    up_far, down_far = along("y", far, 1), along("y", far, 3)
    up_1, down_3 = along("y", up_near[0], 1), along("y", down_near[1], 3)
    up_2, down_2 = along("y", up_far[:half], 1), along("y", down_far[half:], 3)

    quarters = [
        (0, [(1, 0, tokens, from_z[1], 0), (3, 0, tokens, from_z[3], 0), (2, 0, tokens, far, 0)]),
        (3, [(1, 0, tokens, up_near, 0), (3, 0, tokens, up_near, 1), (2, 0, tokens, up_far, 0)]),
        (1, [(1, 0, tokens, down_near, 0), (3, 0, tokens, down_near, 1), (2, 0, tokens, down_far, 0)]),
        (2, [(1, 0, tokens, up_1, 0), (3, 0, tokens, down_3, 0), (2, 0, half, up_2, 0), (2, half, half, down_2, 0)]),
    ]
    grad = jnp.zeros((FF // 128, rows), jnp.float32)
    squares = jnp.float32(0)
    for offset, blocks in quarters:
        q = lax.rem(y + offset, 4)
        others = {}
        for _, _, _, array, _ in blocks:
            if id(array) not in others:
                others[id(array)] = swap(array)
        rights = [(0, 0, 0, tokens, acts, None), (0, 1, 0, tokens, acts_other, None)]
        for group, start, size, array, lead in blocks:
            rights.append((group, 0, start, size, array, lead))
            rights.append((group, 1, start, size, others[id(array)], lead))
        parts = product(jnp.stack([q, x]), left, rights, quarter)
        total = parts[0].astype(jnp.float32)
        for k in (1, 3, 2):
            total = total + along("x", parts[k], k).astype(jnp.float32)
        squares = squares + jnp.sum(total * total)
        grad = lax.dynamic_update_slice_in_dim(grad, total, q * quarter, 1)

    shared = lax.all_to_all(jnp.broadcast_to(squares, (128, 128)), ALL, 0, 0, tiled=True)
    norm = jnp.sqrt(jnp.sum(shared[:, 0]))
    factor = jnp.minimum(1.0, clip_rms * jnp.sqrt(jnp.float32(FF * ROWS)) / norm)
    clipped = factor * grad
    new_moment = beta_first * moment + (1.0 - beta_first) * clipped
    new_second = beta_second * second + (1.0 - beta_second) * clipped * clipped
    new_master = master - learn_rate * new_moment / (jnp.sqrt(new_second) + adam_eps)
    weights = new_master.astype(jnp.bfloat16)
    return (new_moment, new_second, new_master, weights)


def solution(mesh):
    finer = Mesh(mesh.devices.reshape(4, 4, 2, mesh.shape["tensor"]), ALL)
    in_specs = (
        P(DP, None, None),
        P(DP, None, "y"),
        P(DP, None),
        P(DP, None, "y"),
        P(TENSOR_DP, None),
        P(TENSOR_DP, None),
        P(TENSOR_DP, None),
    )
    out_specs = (P(TENSOR_DP, None),) * 4
    return jax.shard_map(per_device, mesh=finer, in_specs=in_specs, out_specs=out_specs, check_vma=False)
```

```python
import functools

import jax
import jax.numpy as jnp
from jax import lax
from jax.experimental import pallas as pl
from jax.experimental.pallas import tpu as pltpu
from jax.sharding import Mesh
from jax.sharding import PartitionSpec as P


FF = 20480
ROWS = 4096
TILE = 128
DP = ("z", "x", "c")
ALL = ("z", "x", "c", "y")
TENSOR_DP = ("y", "z", "x", "c")


clip_rms = 1.0
beta_first = 0.9
beta_second = 0.95
learn_rate = 0.003
adam_eps = 1e-08

SWAP = [(0, 1), (1, 0)]


def ring(shift):
    return [(i, (i + shift) % 4) for i in range(4)]


def along(axis, a, k):
    return lax.ppermute(a, axis, ring(k))


def swap(a):
    return lax.ppermute(a, "c", SWAP)


def widen(act_scale):
    tiles = act_scale.astype(jnp.float32)
    spread = jnp.broadcast_to(tiles[:, :, None], tiles.shape + (TILE,))
    return spread.reshape(tiles.shape[0], tiles.shape[1] * TILE)


def prep_kernel(place_ref, grads_ref, scale_ref, *refs):
    by_z, by_x, turned = refs[:4], refs[4:8], refs[8]
    tokens = grads_ref.shape[0] * grads_ref.shape[1]
    columns = grads_ref.shape[2]
    deq = (grads_ref[...].astype(jnp.float32) * scale_ref[...].astype(jnp.float32)).reshape(tokens, columns)
    turned[...] = deq.T.astype(jnp.bfloat16)
    own = columns // 8
    j = pl.program_id(0)
    z, x, core = place_ref[0], place_ref[1], place_ref[2]
    for k in range(4):

        @pl.when(lax.rem(z + k, 4) == j)
        def _(k=k):
            for at_x in range(4):
                for side in range(2):
                    who = core if side == 0 else 1 - core
                    at = pl.multiple_of((2 * at_x + who) * own, 32)
                    by_z[k][side, at_x * own : (at_x + 1) * own, :] = turned[pl.ds(at, own), :]

        for side in range(2):
            who = core if side == 0 else 1 - core
            at = pl.multiple_of((2 * lax.rem(x + k, 4) + who) * own, 32)
            by_x[k][side, :, :] = turned[pl.ds(at, own), :]


def prep_grads(place, out_grads, grad_scale):
    blocks, tile, columns = out_grads.shape
    tokens = blocks * tile
    part = columns // 4
    shape = jax.ShapeDtypeStruct((2, part // 2, tokens), jnp.bfloat16)
    return pl.pallas_call(
        prep_kernel,
        grid_spec=pltpu.PrefetchScalarGridSpec(
            num_scalar_prefetch=1,
            grid=(4,),
            in_specs=[
                pl.BlockSpec((blocks, tile, part), lambda j, c: (0, 0, j)),
                pl.BlockSpec((blocks, 1, part), lambda j, c: (0, 0, j)),
            ],
            out_specs=[pl.BlockSpec((2, part // 2, tokens), lambda j, c: (0, 0, 0))] * 4
            + [pl.BlockSpec((2, part // 8, tokens), lambda j, c: (0, j, 0))] * 4,
            scratch_shapes=[pltpu.VMEM((part, tokens), jnp.bfloat16)],
        ),
        out_shape=[shape] * 8,
        compiler_params=pltpu.CompilerParams(vmem_limit_bytes=12 * 2**20),
        cost_estimate=pl.CostEstimate(flops=10**9, bytes_accessed=6 * columns * tokens, transcendentals=0),
        name="prep",
    )(place, out_grads, grad_scale)


WHOLE = pl.BlockSpec(memory_space=pltpu.VMEM)
SCALARS = pl.BlockSpec(memory_space=pltpu.SMEM)


def row_block(place_ref, offset, half):
    return 2 * lax.rem(place_ref[3] + offset, 4) + half


def product_kernel(sides, half, offsets, forms, width, place_ref, *refs):
    lefts, refs = refs[: len(sides)], refs[len(sides) :]
    outs, total = refs[-5:-1], refs[-1]
    me = place_ref[1 - half]
    own = total.shape[0] // 4
    for group, form in enumerate(forms):
        at = pl.multiple_of(row_block(place_ref, offsets[group], half) * width, width)
        value = None
        for left, side, (which, lead) in zip(lefts, sides, form):
            cols = refs[which][:, pl.ds(at, width)] if lead is None else refs[which][lead]
            term = jnp.dot(left[side], cols, preferred_element_type=jnp.float32)
            value = term if value is None else value + term
        total[...] = value
        for k in range(4):
            row = pl.multiple_of(lax.rem(me + k, 4) * own, 32)
            outs[k][:, group * width : (group + 1) * width] = total[pl.ds(row, own), :].astype(jnp.bfloat16)


def product(place, half, offsets, lefts, groups, width):
    arrays, forms = [], []
    for rights in groups:
        form = []
        for array, lead in rights:
            known = [i for i, a in enumerate(arrays) if a is array]
            if not known:
                arrays.append(array)
                known = [len(arrays) - 1]
            form.append((known[0], lead))
        forms.append(form)
    columns, tokens = lefts[0][0].shape[1:]
    own = columns // 4
    return pl.pallas_call(
        functools.partial(product_kernel, [side for _, side in lefts], half, offsets, forms, width),
        in_specs=[SCALARS] + [WHOLE] * (len(lefts) + len(arrays)),
        out_specs=[WHOLE] * 4,
        scratch_shapes=[pltpu.VMEM((columns, width), jnp.float32)],
        out_shape=[jax.ShapeDtypeStruct((own, width * len(groups)), jnp.bfloat16)] * 4,
        compiler_params=pltpu.CompilerParams(vmem_limit_bytes=12 * 2**20),
        cost_estimate=pl.CostEstimate(
            flops=2 * columns * 8 * tokens * width * len(groups),
            bytes_accessed=16 * tokens * (columns + width),
            transcendentals=0,
        ),
        name="product",
    )(place, *[a for a, _ in lefts], *arrays)


def folded(squares):
    high, wide = squares.shape
    value = None
    for r in range(0, high, 8):
        for w in range(0, wide, 128):
            term = squares[r : r + 8, w : w + 128]
            value = term if value is None else value + term
    return value


def sums_kernel(count, last, *refs):
    parts, refs = refs[: 4 * count], refs[4 * count :]
    before, refs = (refs[0], refs[1:]) if last else (None, refs)
    squares = before[...] if last else None
    for n in range(count):
        value = parts[4 * n][...].astype(jnp.float32)
        for k in range(1, 4):
            value = value + parts[4 * n + k][...].astype(jnp.float32)
        refs[n][...] = value
        term = folded(value * value)
        squares = term if squares is None else squares + term
    if last:
        refs[count][...] = jnp.broadcast_to(jnp.sum(squares, keepdims=True)[None], refs[count].shape)
    else:
        refs[count][...] = squares


def sums(pieces, before=None):
    last = before is not None
    flat = [p for piece in pieces for p in piece] + ([before] if last else [])
    shapes = [jax.ShapeDtypeStruct(piece[0].shape, jnp.float32) for piece in pieces]
    shapes.append(jax.ShapeDtypeStruct((128, 1, 128) if last else (8, 128), jnp.float32))
    return pl.pallas_call(
        functools.partial(sums_kernel, len(pieces), last),
        in_specs=[WHOLE] * len(flat),
        out_specs=[WHOLE] * len(shapes),
        out_shape=shapes,
        compiler_params=pltpu.CompilerParams(vmem_limit_bytes=12 * 2**20),
        cost_estimate=pl.CostEstimate(flops=10**8, bytes_accessed=4 * 10**6, transcendentals=0),
        name="sums",
    )(*flat)


def adam_kernel(slots, place_ref, shared, *refs):
    grads, refs = refs[:-8], refs[-8:]
    moment, second, master, out_moment, out_second, out_master, out_weights, grad = refs
    step = pl.program_id(0)
    for n, slot in enumerate(slots):

        @pl.when(step == n)
        def _(which=slot[0]):
            grad[...] = grads[which][...]

    norm = jnp.sqrt(jnp.sum(shared[...], axis=0))
    factor = jnp.minimum(1.0, clip_rms * jnp.sqrt(jnp.float32(FF * ROWS)) / norm)
    clipped = factor[0:1, 0:1] * grad[...]
    new_moment = beta_first * moment[...] + (1.0 - beta_first) * clipped
    new_second = beta_second * second[...] + (1.0 - beta_second) * clipped * clipped
    new_master = master[...] - learn_rate * new_moment / (jnp.sqrt(new_second) + adam_eps)
    out_moment[...] = new_moment
    out_second[...] = new_second
    out_master[...] = new_master
    out_weights[...] = new_master.astype(jnp.bfloat16)


def adam(place, slots, piece, shared, grads, moment, second, master):
    own, rows = moment.shape

    def at(j, place_ref):
        block = row_block(place_ref, *slots[0][2:])
        for n, slot in enumerate(slots[1:], 1):
            block = jnp.where(j == n, row_block(place_ref, *slot[2:]), block)
        return 0, block

    firsts = [min(n for n, slot in enumerate(slots) if slot[0] == i) for i in range(len(grads))]
    block = pl.BlockSpec((own, piece), at)
    wide = jax.ShapeDtypeStruct((own, rows), jnp.float32)
    return pl.pallas_call(
        functools.partial(adam_kernel, slots),
        grid_spec=pltpu.PrefetchScalarGridSpec(
            num_scalar_prefetch=1,
            grid=(len(slots),),
            in_specs=[pl.BlockSpec(shared.shape, lambda j, p: (0, 0, 0))]
            + [
                pl.BlockSpec(
                    (own, piece), lambda j, p, n=n, last=g.shape[1] // piece - 1: (0, jnp.clip(j - n, 0, last))
                )
                for n, g in zip(firsts, grads)
            ]
            + [block] * 3,
            out_specs=[block] * 4,
            scratch_shapes=[pltpu.VMEM((own, piece), jnp.float32)],
        ),
        out_shape=[wide, wide, wide, jax.ShapeDtypeStruct((own, rows), jnp.bfloat16)],
        compiler_params=pltpu.CompilerParams(vmem_limit_bytes=60 * 2**20),
        cost_estimate=pl.CostEstimate(flops=10**7, bytes_accessed=17 * 10**6, transcendentals=10**6),
        name="adam",
    )(place, shared, *grads, moment, second, master)


def step(activations, out_grads, act_scale, grad_scale, moment, second, master):
    z, x, c, y = (lax.axis_index(a).astype(jnp.int32) for a in ("z", "x", "c", "y"))
    place = jnp.stack([z, x, c, y])
    rows = activations.shape[2]
    quarter = rows // 4
    piece = quarter // 2
    tokens = activations.shape[0] * activations.shape[1]

    acts = (
        (activations.astype(jnp.float32) * widen(act_scale)[:, None, :]).astype(jnp.bfloat16).reshape(tokens, rows)
    )
    slabs = [lax.dynamic_slice_in_dim(acts, y * quarter + h * piece, piece, 1) for h in range(2)]
    gather_axis, reduce_axis = ("z", "x"), ("x", "z")

    near = [{k: along(gather_axis[h], slabs[h], k) for k in (1, 2, 3)} for h in range(2)]
    acts_other = swap(acts)

    blocks = prep_grads(place, out_grads, grad_scale)
    sent = [blocks[:4], blocks[4:]]
    arrived = [[sent[h][0]] + [along(gather_axis[h], sent[h][k], k) for k in (1, 2, 3)] for h in range(2)]
    lefts = [[p for a in arrived[h] for p in ((a, 0), (swap(a), 1))] for h in range(2)]

    held = [jnp.stack([near[h][k] for k in (1, 2, 3)]) for h in range(2)]
    up = [along("y", held[h], 1) for h in range(2)]
    down = [along("y", held[h], 3) for h in range(2)]
    across = [along("y", up[0], 1), along("y", down[1], 3)]

    pieces, slots = [], []
    for stage in ([(0, held)], [(3, up), (1, down)], [(2, across)]):
        for h in range(2):
            groups = []
            for n, (offset, source) in enumerate(stage):
                own, other = source[h], swap(source[h])
                rights = [(acts, None), (acts_other, None)]
                for lead in range(3):
                    rights += [(own, lead), (other, lead)]
                groups.append(rights)
                slots.append((len(pieces), n, offset, h))
            parts = product(place, h, [offset for offset, _ in stage], lefts[h], groups, piece)
            pieces.append([parts[0]] + [along(reduce_axis[h], parts[k], k) for k in (1, 2, 3)])

    *first, squares = sums(pieces[:4])
    *second_part, squares = sums(pieces[4:], squares)
    shared = lax.all_to_all(squares, ALL, 0, 0, tiled=True)
    return tuple(adam(place, slots, piece, shared, first + second_part, moment, second, master))


def solution(mesh):
    finer = Mesh(mesh.devices.reshape(4, 4, 2, mesh.shape["tensor"]), ALL)
    in_specs = (
        P(DP, None, None),
        P(DP, None, "y"),
        P(DP, None),
        P(DP, None, "y"),
        P(TENSOR_DP, None),
        P(TENSOR_DP, None),
        P(TENSOR_DP, None),
    )
    out_specs = (P(TENSOR_DP, None),) * 4
    return jax.shard_map(step, mesh=finer, in_specs=in_specs, out_specs=out_specs, check_vma=False)
```

```python
import functools

import jax
import jax.numpy as jnp
from jax import lax
from jax.experimental import pallas as pl
from jax.experimental.pallas import tpu as pltpu
from jax.sharding import Mesh
from jax.sharding import PartitionSpec as P


FF = 20480
ROWS = 4096
TILE = 128
DP = ("z", "x", "c")
ALL = ("z", "x", "c", "y")
TENSOR_DP = ("y", "z", "x", "c")


clip_rms = 1.0
beta_first = 0.9
beta_second = 0.95
learn_rate = 0.003
adam_eps = 1e-08

SWAP = [(0, 1), (1, 0)]
WHOLE = pl.BlockSpec(memory_space=pltpu.VMEM)
SCALARS = pl.BlockSpec(memory_space=pltpu.SMEM)


def ring(shift):
    return [(i, (i + shift) % 4) for i in range(4)]


def crossed(shift, first_over_z):
    pairs = []
    for z in range(4):
        for x in range(4):
            for c in range(2):
                over_z = (c == 0) == first_over_z
                to = ((z + shift) % 4, x) if over_z else (z, (x + shift) % 4)
                pairs.append(((z * 4 + x) * 2 + c, (to[0] * 4 + to[1]) * 2 + c))
    return pairs


def gathered(a, k):
    return lax.ppermute(a, DP, crossed(k, True))


def scattered(a, k):
    return lax.ppermute(a, DP, crossed(k, False))


def along_y(a, k):
    return lax.ppermute(a, "y", ring(k))


def swapped(a):
    return lax.ppermute(a, "c", SWAP)


def gather_at(place_ref):
    return jnp.where(place_ref[2] == 0, place_ref[0], place_ref[1])


def reduce_at(place_ref):
    return jnp.where(place_ref[2] == 0, place_ref[1], place_ref[0])


def dequantized(acts_ref, scale_ref, at):
    blocks, tile, width = acts_ref.shape
    scales = scale_ref[...].astype(jnp.float32)
    lane = lax.broadcasted_iota(jnp.int32, scales.shape, 1)
    strips = []
    for t in range(width // TILE):
        chosen = jnp.sum(jnp.where(lane == at * (width // TILE) + t, scales, 0.0), axis=1, keepdims=True)
        strip = acts_ref[:, :, t * TILE : (t + 1) * TILE].astype(jnp.float32) * chosen[:, :, None]
        strips.append(strip.astype(jnp.bfloat16).reshape(blocks * tile, TILE))
    return strips


def slab_kernel(place_ref, mine_ref, theirs_ref, scale_ref, *outs):
    core, y = place_ref[2], place_ref[3]
    for source, at, out in ((mine_ref, 2 * y + core, outs[0]), (theirs_ref, 2 * y + 1 - core, outs[1])):
        for t, strip in enumerate(dequantized(source, scale_ref, at)):
            out[:, t * TILE : (t + 1) * TILE] = strip


def slab(place, activations, act_scale):
    blocks, tile, rows = activations.shape
    piece = rows // 8
    shape = jax.ShapeDtypeStruct((blocks * tile, piece), jnp.bfloat16)
    acts = pltpu.with_memory_space_constraint(activations, pltpu.HBM)
    return pl.pallas_call(
        slab_kernel,
        grid_spec=pltpu.PrefetchScalarGridSpec(
            num_scalar_prefetch=1,
            grid=(1,),
            in_specs=[
                pl.BlockSpec((blocks, tile, piece), lambda j, p: (0, 0, 2 * p[3] + p[2])),
                pl.BlockSpec((blocks, tile, piece), lambda j, p: (0, 0, 2 * p[3] + 1 - p[2])),
                pl.BlockSpec(act_scale.shape, lambda j, p: (0, 0)),
            ],
            out_specs=[pl.BlockSpec(shape.shape, lambda j, p: (0, 0))] * 2,
        ),
        out_shape=[shape, shape],
        compiler_params=pltpu.CompilerParams(vmem_limit_bytes=8 * 2**20),
        cost_estimate=pl.CostEstimate(flops=10**6, bytes_accessed=10**6, transcendentals=0),
        name="slab",
    )(place, acts, acts, act_scale)


def acts_kernel(place_ref, own_ref, other_ref, own_scale_ref, other_scale_ref, whole_ref, opposite_ref):
    j = pl.program_id(0)
    tokens = whole_ref.shape[0] // 2
    at = 2 * j + place_ref[2]
    for n, (source, scale) in enumerate(((own_ref, own_scale_ref), (other_ref, other_scale_ref))):
        for t, strip in enumerate(dequantized(source, scale, at)):
            whole_ref[n * tokens : (n + 1) * tokens, t * TILE : (t + 1) * TILE] = strip

    @pl.when(lax.rem(place_ref[3] + 2, 4) == j)
    def _():
        opposite_ref[...] = whole_ref[...]


def all_acts(place, own, other, own_scale, other_scale):
    blocks, tile, rows = own.shape
    tokens, piece = 2 * blocks * tile, rows // 8
    block = pl.BlockSpec((blocks, tile, piece), lambda j, p: (0, 0, 2 * j + p[2]))
    scale = pl.BlockSpec(own_scale.shape, lambda j, p: (0, 0))
    return pl.pallas_call(
        acts_kernel,
        grid_spec=pltpu.PrefetchScalarGridSpec(
            num_scalar_prefetch=1,
            grid=(4,),
            in_specs=[block, block, scale, scale],
            out_specs=[
                pl.BlockSpec((tokens, piece), lambda j, p: (0, j)),
                pl.BlockSpec((tokens, piece), lambda j, p: (0, 0)),
            ],
        ),
        out_shape=[
            jax.ShapeDtypeStruct((tokens, 4 * piece), jnp.bfloat16),
            jax.ShapeDtypeStruct((tokens, piece), jnp.bfloat16),
        ],
        compiler_params=pltpu.CompilerParams(vmem_limit_bytes=8 * 2**20),
        cost_estimate=pl.CostEstimate(flops=10**6, bytes_accessed=4 * 10**6, transcendentals=0),
        name="acts",
    )(place, pltpu.with_memory_space_constraint(own, pltpu.HBM), other, own_scale, other_scale)


def prep_kernel(place_ref, own_ref, other_ref, own_scale_ref, other_scale_ref, *refs):
    outs, turned = refs[:4], refs[4]
    tokens = own_ref.shape[0] * own_ref.shape[1]
    columns = own_ref.shape[2]
    for n, (source, scale) in enumerate(((own_ref, own_scale_ref), (other_ref, other_scale_ref))):
        deq = (source[...].astype(jnp.float32) * scale[...].astype(jnp.float32)).reshape(tokens, columns)
        turned[:, n * tokens : (n + 1) * tokens] = deq.T.astype(jnp.bfloat16)
    both = columns // 4
    j = pl.program_id(0)
    me = gather_at(place_ref)
    for k in range(4):
        to = lax.rem(me + k, 4)

        @pl.when(jnp.logical_and(place_ref[2] == 0, to == j))
        def _(k=k):
            outs[k][...] = turned[...]

        @pl.when(place_ref[2] == 1)
        def _(k=k, to=to):
            at = pl.multiple_of(to * both, 32)
            outs[k][pl.ds(pl.multiple_of(j * both, 32), both), :] = turned[pl.ds(at, both), :]


def prep_grads(place, own, other, own_scale, other_scale):
    blocks, tile, columns = own.shape
    tokens = blocks * tile
    part = columns // 4
    shape = jax.ShapeDtypeStruct((part, 2 * tokens), jnp.bfloat16)
    block = pl.BlockSpec((blocks, tile, part), lambda j, p: (0, 0, j))
    scale = pl.BlockSpec((blocks, 1, part), lambda j, p: (0, 0, j))
    return pl.pallas_call(
        prep_kernel,
        grid_spec=pltpu.PrefetchScalarGridSpec(
            num_scalar_prefetch=1,
            grid=(4,),
            in_specs=[block, block, scale, scale],
            out_specs=[pl.BlockSpec(shape.shape, lambda j, p: (0, 0))] * 4,
            scratch_shapes=[pltpu.VMEM(shape.shape, jnp.bfloat16)],
        ),
        out_shape=[shape] * 4,
        compiler_params=pltpu.CompilerParams(vmem_limit_bytes=20 * 2**20),
        cost_estimate=pl.CostEstimate(flops=10**9, bytes_accessed=8 * columns * tokens, transcendentals=0),
        name="prep",
    )(place, pltpu.with_memory_space_constraint(own, pltpu.HBM), other, own_scale, other_scale)


def product_kernel(offsets, forms, width, place_ref, *refs):
    lefts, refs = refs[:4], refs[4:]
    outs, total = refs[-5:-1], refs[-1]
    me = reduce_at(place_ref)
    columns = total.shape[0]
    both = columns // 4
    for group, form in enumerate(forms):
        at = pl.multiple_of(lax.rem(place_ref[3] + offsets[group], 4) * width, width)
        for start in range(0, columns, columns // 2):
            value = None
            for left, (which, lead) in zip(lefts, form):
                if which == 0:
                    cols = refs[0][:, pl.ds(at, width)]
                else:
                    cols = refs[which][...] if lead is None else refs[which][lead]
                term = jnp.dot(left[start : start + columns // 2, :], cols, preferred_element_type=jnp.float32)
                value = term if value is None else value + term
            total[start : start + columns // 2, :] = value
        for k in range(4):
            row = pl.multiple_of(lax.rem(me + k, 4) * both, 32)
            outs[k][:, group * width : (group + 1) * width] = total[pl.ds(row, both), :].astype(jnp.bfloat16)


def product(place, offsets, lefts, acts, groups, width):
    arrays, forms = [acts], []
    for rights in groups:
        form = [(0, None)]
        for array, lead in rights:
            known = [i for i, a in enumerate(arrays) if a is array]
            if not known:
                arrays.append(array)
                known = [len(arrays) - 1]
            form.append((known[0], lead))
        forms.append(form)
    columns, tokens = lefts[0].shape
    both = columns // 4
    return pl.pallas_call(
        functools.partial(product_kernel, offsets, forms, width),
        in_specs=[SCALARS] + [WHOLE] * (4 + len(arrays)),
        out_specs=[WHOLE] * 4,
        scratch_shapes=[pltpu.VMEM((columns, width), jnp.float32)],
        out_shape=[jax.ShapeDtypeStruct((both, width * len(groups)), jnp.bfloat16)] * 4,
        compiler_params=pltpu.CompilerParams(vmem_limit_bytes=12 * 2**20),
        cost_estimate=pl.CostEstimate(
            flops=8 * columns * tokens * width * len(groups),
            bytes_accessed=8 * tokens * (columns + width),
            transcendentals=0,
        ),
        name="product",
    )(place, *lefts, *arrays)


def folded(squares):
    high, wide = squares.shape
    value = None
    for r in range(0, high, 8):
        for w in range(0, wide, 128):
            term = squares[r : r + 8, w : w + 128]
            value = term if value is None else value + term
    return value


def sums_kernel(count, last, place_ref, *refs):
    parts, refs = refs[: 4 * count], refs[4 * count :]
    before, refs = (refs[0], refs[1:]) if last else (None, refs)
    squares = before[...] if last else None
    own = refs[0].shape[0]
    core = place_ref[2]
    for n in range(count):
        for side in range(2):
            who = core if side == 0 else 1 - core
            at = pl.ds(pl.multiple_of(who * own, 32), own)
            value = parts[4 * n][at, :].astype(jnp.float32)
            for k in range(1, 4):
                value = value + parts[4 * n + k][at, :].astype(jnp.float32)
            refs[2 * n + side][...] = value
            term = folded(value * value)
            squares = term if squares is None else squares + term
    if last:
        refs[-1][...] = jnp.broadcast_to(jnp.sum(squares, keepdims=True)[None], refs[-1].shape)
    else:
        refs[-1][...] = squares


def sums(place, pieces, before=None):
    last = before is not None
    flat = [p for piece in pieces for p in piece] + ([before] if last else [])
    shapes = []
    for piece in pieces:
        both, width = piece[0].shape
        shapes += [pltpu.HBM((both // 2, width), jnp.float32)] * 2
    shapes.append(jax.ShapeDtypeStruct((128, 1, 128) if last else (8, 128), jnp.float32))
    *values, squares = pl.pallas_call(
        functools.partial(sums_kernel, len(pieces), last),
        in_specs=[SCALARS] + [WHOLE] * len(flat),
        out_specs=[WHOLE] * len(shapes),
        out_shape=shapes,
        compiler_params=pltpu.CompilerParams(vmem_limit_bytes=8 * 2**20),
        cost_estimate=pl.CostEstimate(flops=10**8, bytes_accessed=4 * 10**6, transcendentals=0),
        name="sums",
    )(place, *flat)
    return values[::2], values[1::2], squares


def adam_kernel(slots, place_ref, shared, *refs):
    grads, refs = refs[:-8], refs[-8:]
    moment, second, master, out_moment, out_second, out_master, out_weights, grad = refs
    step = pl.program_id(0)
    wide = grad.shape[1] // 2
    core = place_ref[2]
    for n, (_, which, _) in enumerate(slots):

        @pl.when(step == n)
        def _(which=which):
            grad[:, pl.ds(pl.multiple_of(core * wide, wide), wide)] = grads[2 * which][...]
            grad[:, pl.ds(pl.multiple_of((1 - core) * wide, wide), wide)] = grads[2 * which + 1][...]

    norm = jnp.sqrt(jnp.sum(shared[...], axis=0))
    factor = jnp.minimum(1.0, clip_rms * jnp.sqrt(jnp.float32(FF * ROWS)) / norm)
    clipped = factor[0:1, 0:1] * grad[...]
    new_moment = beta_first * moment[...] + (1.0 - beta_first) * clipped
    new_second = beta_second * second[...] + (1.0 - beta_second) * clipped * clipped
    new_master = master[...] - learn_rate * new_moment / (jnp.sqrt(new_second) + adam_eps)
    out_moment[...] = new_moment
    out_second[...] = new_second
    out_master[...] = new_master
    out_weights[...] = new_master.astype(jnp.bfloat16)


def chosen(j, values):
    found = values[0]
    for n, value in enumerate(values[1:], 1):
        found = jnp.where(j == n, value, found)
    return found


def adam(place, slots, shared, pairs, moment, second, master):
    own, rows = moment.shape
    quarter = rows // 4
    block = pl.BlockSpec((own, quarter), lambda j, p: (0, lax.rem(p[3] + chosen(j, [s[0] for s in slots]), 4)))

    def source(i):
        at, blocks = 0, []
        for _, which, lead in slots:
            at = lead if which == i else at
            blocks.append(at)
        return [pl.BlockSpec((own, quarter // 2), lambda j, p: (0, chosen(j, blocks)))] * 2

    wide = jax.ShapeDtypeStruct((own, rows), jnp.float32)
    return pl.pallas_call(
        functools.partial(adam_kernel, slots),
        grid_spec=pltpu.PrefetchScalarGridSpec(
            num_scalar_prefetch=1,
            grid=(len(slots),),
            in_specs=[pl.BlockSpec(shared.shape, lambda j, p: (0, 0, 0))]
            + [spec for i in range(len(pairs)) for spec in source(i)]
            + [block] * 3,
            out_specs=[block] * 4,
            scratch_shapes=[pltpu.VMEM((own, quarter), jnp.float32)],
        ),
        out_shape=[wide, wide, wide, jax.ShapeDtypeStruct((own, rows), jnp.bfloat16)],
        compiler_params=pltpu.CompilerParams(vmem_limit_bytes=60 * 2**20),
        cost_estimate=pl.CostEstimate(flops=10**7, bytes_accessed=17 * 10**6, transcendentals=10**6),
        name="adam",
    )(place, shared, *[a for pair in pairs for a in pair], moment, second, master)


PRODUCTS = ((0,), (3, 1), (2,))
EARLY = 2


def step(activations, out_grads, act_scale, grad_scale, moment, second, master):
    place = jnp.stack([lax.axis_index(a).astype(jnp.int32) for a in ("z", "x", "c", "y")])
    piece = activations.shape[2] // 8

    mine, theirs = slab(place, activations, act_scale)
    held_own = jnp.concatenate([mine, swapped(theirs)], 0)
    near = [gathered(held_own, k) for k in (1, 2, 3)]

    lefts = prep_grads(place, out_grads, swapped(out_grads), grad_scale, swapped(grad_scale))
    lefts = [lefts[0]] + [gathered(lefts[k], k) for k in (1, 2, 3)]

    acts, opposite = all_acts(place, activations, swapped(activations), act_scale, swapped(act_scale))

    held = jnp.stack(near)
    across = [gathered(opposite, k) for k in (1, 2, 3)]
    sources = {0: held, 3: along_y(held, 1), 1: along_y(held, 3)}
    rights = {offset: [(array, lead) for lead in range(3)] for offset, array in sources.items()}
    rights[2] = [(array, None) for array in across]

    pieces, slots = [], []
    for number, offsets in enumerate(PRODUCTS):
        slots += [(offset, number, n) for n, offset in enumerate(offsets)]
        parts = product(place, offsets, lefts, acts, [rights[offset] for offset in offsets], piece)
        pieces.append([parts[0]] + [scattered(parts[k], k) for k in (1, 2, 3)])

    kept, given, squares = sums(place, pieces[:EARLY])
    more_kept, more_given, squares = sums(place, pieces[EARLY:], squares)
    kept, given = kept + more_kept, given + more_given
    pairs = [(own, pltpu.with_memory_space_constraint(swapped(other), pltpu.HBM)) for own, other in zip(kept, given)]
    shared = lax.all_to_all(squares, ALL, 0, 0, tiled=True)
    return tuple(adam(place, slots, shared, pairs, moment, second, master))


def solution(mesh):
    finer = Mesh(mesh.devices.reshape(4, 4, 2, mesh.shape["tensor"]), ALL)
    in_specs = (
        P(DP, None, None),
        P(DP, None, "y"),
        P(DP, None),
        P(DP, None, "y"),
        P(TENSOR_DP, None),
        P(TENSOR_DP, None),
        P(TENSOR_DP, None),
    )
    out_specs = (P(TENSOR_DP, None),) * 4
    return jax.shard_map(step, mesh=finer, in_specs=in_specs, out_specs=out_specs, check_vma=False)
```

```python
import functools

import jax
import jax.numpy as jnp
from jax import lax
from jax.experimental import pallas as pl
from jax.experimental.pallas import tpu as pltpu
from jax.sharding import Mesh
from jax.sharding import PartitionSpec as P


FF = 20480
ROWS = 4096
TILE = 128
DP = ("z", "x", "c")
ALL = ("z", "x", "c", "y")
TENSOR_DP = ("y", "z", "x", "c")


clip_rms = 1.0
beta_first = 0.9
beta_second = 0.95
learn_rate = 0.003
adam_eps = 1e-08

SWAP = [(0, 1), (1, 0)]
WHOLE = pl.BlockSpec(memory_space=pltpu.VMEM)
SCALARS = pl.BlockSpec(memory_space=pltpu.SMEM)


def ring(shift):
    return [(i, (i + shift) % 4) for i in range(4)]


def crossed(shift, first_over_z):
    pairs = []
    for z in range(4):
        for x in range(4):
            for c in range(2):
                over_z = (c == 0) == first_over_z
                to = ((z + shift) % 4, x) if over_z else (z, (x + shift) % 4)
                pairs.append(((z * 4 + x) * 2 + c, (to[0] * 4 + to[1]) * 2 + c))
    return pairs


def gathered(a, k):
    return lax.ppermute(a, DP, crossed(k, True))


def scattered(a, k):
    return lax.ppermute(a, DP, crossed(k, False))


def along_y(a, k):
    return lax.ppermute(a, "y", ring(k))


def swapped(a):
    return lax.ppermute(a, "c", SWAP)


def gather_at(place_ref):
    return jnp.where(place_ref[2] == 0, place_ref[0], place_ref[1])


def reduce_at(place_ref):
    return jnp.where(place_ref[2] == 0, place_ref[1], place_ref[0])


def dequantized(acts_ref, scale_ref, at):
    blocks, tile, width = acts_ref.shape
    scales = scale_ref[...].astype(jnp.float32)
    lane = lax.broadcasted_iota(jnp.int32, scales.shape, 1)
    strips = []
    for t in range(width // TILE):
        chosen = jnp.sum(jnp.where(lane == at * (width // TILE) + t, scales, 0.0), axis=1, keepdims=True)
        strip = acts_ref[:, :, t * TILE : (t + 1) * TILE].astype(jnp.float32) * chosen[:, :, None]
        strips.append(strip.astype(jnp.bfloat16).reshape(blocks * tile, TILE))
    return strips


def slab_kernel(place_ref, mine_ref, theirs_ref, scale_ref, *outs):
    core, y = place_ref[2], place_ref[3]
    for source, at, out in ((mine_ref, 2 * y + core, outs[0]), (theirs_ref, 2 * y + 1 - core, outs[1])):
        for t, strip in enumerate(dequantized(source, scale_ref, at)):
            out[:, t * TILE : (t + 1) * TILE] = strip


def slab(place, activations, act_scale):
    blocks, tile, rows = activations.shape
    piece = rows // 8
    shape = jax.ShapeDtypeStruct((blocks * tile, piece), jnp.bfloat16)
    acts = pltpu.with_memory_space_constraint(activations, pltpu.HBM)
    return pl.pallas_call(
        slab_kernel,
        grid_spec=pltpu.PrefetchScalarGridSpec(
            num_scalar_prefetch=1,
            grid=(1,),
            in_specs=[
                pl.BlockSpec((blocks, tile, piece), lambda j, p: (0, 0, 2 * p[3] + p[2])),
                pl.BlockSpec((blocks, tile, piece), lambda j, p: (0, 0, 2 * p[3] + 1 - p[2])),
                pl.BlockSpec(act_scale.shape, lambda j, p: (0, 0)),
            ],
            out_specs=[pl.BlockSpec(shape.shape, lambda j, p: (0, 0))] * 2,
        ),
        out_shape=[shape, shape],
        compiler_params=pltpu.CompilerParams(vmem_limit_bytes=8 * 2**20),
        cost_estimate=pl.CostEstimate(flops=10**6, bytes_accessed=10**6, transcendentals=0),
        name="slab",
    )(place, acts, acts, pltpu.with_memory_space_constraint(act_scale, pltpu.HBM))


def acts_kernel(place_ref, own_ref, other_ref, own_scale_ref, other_scale_ref, whole_ref, opposite_ref):
    j = pl.program_id(0)
    tokens = whole_ref.shape[0] // 2
    at = 2 * j + place_ref[2]
    for n, (source, scale) in enumerate(((own_ref, own_scale_ref), (other_ref, other_scale_ref))):
        for t, strip in enumerate(dequantized(source, scale, at)):
            whole_ref[n * tokens : (n + 1) * tokens, t * TILE : (t + 1) * TILE] = strip

    @pl.when(lax.rem(place_ref[3] + 2, 4) == j)
    def _():
        opposite_ref[...] = whole_ref[...]


def all_acts(place, own, other, own_scale, other_scale):
    blocks, tile, rows = own.shape
    tokens, piece = 2 * blocks * tile, rows // 8
    block = pl.BlockSpec((blocks, tile, piece), lambda j, p: (0, 0, 2 * j + p[2]))
    scale = pl.BlockSpec(own_scale.shape, lambda j, p: (0, 0))
    return pl.pallas_call(
        acts_kernel,
        grid_spec=pltpu.PrefetchScalarGridSpec(
            num_scalar_prefetch=1,
            grid=(4,),
            in_specs=[block, block, scale, scale],
            out_specs=[
                pl.BlockSpec((tokens, piece), lambda j, p: (0, j)),
                pl.BlockSpec((tokens, piece), lambda j, p: (0, 0)),
            ],
        ),
        out_shape=[
            jax.ShapeDtypeStruct((tokens, 4 * piece), jnp.bfloat16),
            jax.ShapeDtypeStruct((tokens, piece), jnp.bfloat16),
        ],
        compiler_params=pltpu.CompilerParams(vmem_limit_bytes=8 * 2**20),
        cost_estimate=pl.CostEstimate(flops=10**6, bytes_accessed=4 * 10**6, transcendentals=0),
        name="acts",
    )(place, pltpu.with_memory_space_constraint(own, pltpu.HBM), other, own_scale, other_scale)


def prep_kernel(place_ref, own_ref, other_ref, own_scale_ref, other_scale_ref, *refs):
    outs, turned = refs[:4], refs[4]
    tokens = own_ref.shape[0] * own_ref.shape[1]
    columns = own_ref.shape[2]
    for n, (source, scale) in enumerate(((own_ref, own_scale_ref), (other_ref, other_scale_ref))):
        deq = (source[...].astype(jnp.float32) * scale[...].astype(jnp.float32)).reshape(tokens, columns)
        turned[:, n * tokens : (n + 1) * tokens] = deq.T.astype(jnp.bfloat16)
    both = columns // 4
    j = pl.program_id(0)
    me = gather_at(place_ref)
    for k in range(4):
        to = lax.rem(me + k, 4)

        @pl.when(jnp.logical_and(place_ref[2] == 0, to == j))
        def _(k=k):
            outs[k][...] = turned[...]

        @pl.when(place_ref[2] == 1)
        def _(k=k, to=to):
            at = pl.multiple_of(to * both, 32)
            outs[k][pl.ds(pl.multiple_of(j * both, 32), both), :] = turned[pl.ds(at, both), :]


def prep_grads(place, own, other, own_scale, other_scale):
    blocks, tile, columns = own.shape
    tokens = blocks * tile
    part = columns // 4
    shape = jax.ShapeDtypeStruct((part, 2 * tokens), jnp.bfloat16)
    block = pl.BlockSpec((blocks, tile, part), lambda j, p: (0, 0, j))
    scale = pl.BlockSpec((blocks, 1, part), lambda j, p: (0, 0, j))
    return pl.pallas_call(
        prep_kernel,
        grid_spec=pltpu.PrefetchScalarGridSpec(
            num_scalar_prefetch=1,
            grid=(4,),
            in_specs=[block, block, scale, scale],
            out_specs=[pl.BlockSpec(shape.shape, lambda j, p: (0, 0))] * 4,
            scratch_shapes=[pltpu.VMEM(shape.shape, jnp.bfloat16)],
        ),
        out_shape=[shape] * 4,
        compiler_params=pltpu.CompilerParams(vmem_limit_bytes=20 * 2**20),
        cost_estimate=pl.CostEstimate(flops=10**9, bytes_accessed=8 * columns * tokens, transcendentals=0),
        name="prep",
    )(place, pltpu.with_memory_space_constraint(own, pltpu.HBM), other, own_scale, other_scale)


def product_kernel(offsets, forms, width, place_ref, *refs):
    lefts, refs = refs[:4], refs[4:]
    outs, total = refs[-5:-1], refs[-1]
    me = reduce_at(place_ref)
    columns = total.shape[0]
    both = columns // 4
    for group, form in enumerate(forms):
        at = pl.multiple_of(lax.rem(place_ref[3] + offsets[group], 4) * width, width)
        for start in range(0, columns, columns // 2):
            value = None
            for left, (which, lead) in zip(lefts, form):
                if which == 0:
                    cols = refs[0][:, pl.ds(at, width)]
                else:
                    cols = refs[which][...] if lead is None else refs[which][lead]
                term = jnp.dot(left[start : start + columns // 2, :], cols, preferred_element_type=jnp.float32)
                value = term if value is None else value + term
            total[start : start + columns // 2, :] = value
        for k in range(4):
            row = pl.multiple_of(lax.rem(me + k, 4) * both, 32)
            outs[k][:, group * width : (group + 1) * width] = total[pl.ds(row, both), :].astype(jnp.bfloat16)


def product(place, offsets, lefts, acts, groups, width):
    arrays, forms = [acts], []
    for rights in groups:
        form = [(0, None)]
        for array, lead in rights:
            known = [i for i, a in enumerate(arrays) if a is array]
            if not known:
                arrays.append(array)
                known = [len(arrays) - 1]
            form.append((known[0], lead))
        forms.append(form)
    columns, tokens = lefts[0].shape
    both = columns // 4
    return pl.pallas_call(
        functools.partial(product_kernel, offsets, forms, width),
        in_specs=[SCALARS] + [WHOLE] * (4 + len(arrays)),
        out_specs=[WHOLE] * 4,
        scratch_shapes=[pltpu.VMEM((columns, width), jnp.float32)],
        out_shape=[jax.ShapeDtypeStruct((both, width * len(groups)), jnp.bfloat16)] * 4,
        compiler_params=pltpu.CompilerParams(vmem_limit_bytes=12 * 2**20),
        cost_estimate=pl.CostEstimate(
            flops=8 * columns * tokens * width * len(groups),
            bytes_accessed=8 * tokens * (columns + width),
            transcendentals=0,
        ),
        name="product",
    )(place, *lefts, *arrays)


def folded(squares):
    high, wide = squares.shape
    value = None
    for r in range(0, high, 8):
        for w in range(0, wide, 128):
            term = squares[r : r + 8, w : w + 128]
            value = term if value is None else value + term
    return value


def sums_kernel(count, last, place_ref, *refs):
    parts, refs = refs[: 4 * count], refs[4 * count :]
    before, refs = (refs[0], refs[1:]) if last else (None, refs)
    squares = before[...] if last else None
    own = refs[0].shape[0]
    core = place_ref[2]
    for n in range(count):
        for side in range(2):
            who = core if side == 0 else 1 - core
            at = pl.ds(pl.multiple_of(who * own, 32), own)
            value = parts[4 * n][at, :].astype(jnp.float32)
            for k in range(1, 4):
                value = value + parts[4 * n + k][at, :].astype(jnp.float32)
            refs[2 * n + side][...] = value.astype(jnp.bfloat16)
            term = folded(value * value)
            squares = term if squares is None else squares + term
    if last:
        refs[-1][...] = jnp.broadcast_to(jnp.sum(squares, keepdims=True)[None], refs[-1].shape)
    else:
        refs[-1][...] = squares


def sums(place, pieces, before=None):
    last = before is not None
    flat = [p for piece in pieces for p in piece] + ([before] if last else [])
    shapes = []
    for piece in pieces:
        both, width = piece[0].shape
        shapes += [pltpu.HBM((both // 2, width), jnp.bfloat16)] * 2
    shapes.append(jax.ShapeDtypeStruct((128, 1, 128) if last else (8, 128), jnp.float32))
    *values, squares = pl.pallas_call(
        functools.partial(sums_kernel, len(pieces), last),
        in_specs=[SCALARS] + [WHOLE] * len(flat),
        out_specs=[WHOLE] * len(shapes),
        out_shape=shapes,
        compiler_params=pltpu.CompilerParams(vmem_limit_bytes=8 * 2**20),
        cost_estimate=pl.CostEstimate(flops=10**8, bytes_accessed=4 * 10**6, transcendentals=0),
        name="sums",
    )(place, *flat)
    return values[::2], values[1::2], squares


def adam_kernel(slots, place_ref, shared, *refs):
    count = 2 * len({which for _, which, _ in slots})
    grads, refs = refs[:count], refs[count:]
    sources, targets = refs[:3], refs[3:7]
    grad_in, read, written, weights_out, in_sems, out_sems = refs[7:]
    piece = grad_in.shape[2]
    core, y = place_ref[2], place_ref[3]
    blocks = [(offset, which, lead, side) for offset, which, lead in slots for side in range(2)]
    ats, fetches = [], []
    for n, (offset, which, lead, side) in enumerate(blocks):
        half = core if side == 0 else 1 - core
        at = pl.ds(pl.multiple_of((2 * lax.rem(y + offset, 4) + half) * piece, piece), piece)
        ats.append(at)
        from_grad = grads[2 * which + side].at[:, lead * piece : (lead + 1) * piece]
        copies = [pltpu.make_async_copy(from_grad, grad_in.at[n], in_sems.at[n, 3])]
        for i, source in enumerate(sources):
            copies.append(pltpu.make_async_copy(source.at[:, at], read.at[n, i], in_sems.at[n, i]))
        for copy in copies:
            copy.start()
        fetches.append(copies)

    norm = jnp.sqrt(jnp.sum(shared[...], axis=0))
    factor = jnp.minimum(1.0, clip_rms * jnp.sqrt(jnp.float32(FF * ROWS)) / norm)
    stores = []
    for n, at in enumerate(ats):
        for copy in fetches[n]:
            copy.wait()
        clipped = factor[0:1, 0:1] * grad_in[n].astype(jnp.float32)
        new_moment = beta_first * read[n, 0] + (1.0 - beta_first) * clipped
        new_second = beta_second * read[n, 1] + (1.0 - beta_second) * clipped * clipped
        new_master = read[n, 2] - learn_rate * new_moment / (jnp.sqrt(new_second) + adam_eps)
        written[n, 0] = new_moment
        written[n, 1] = new_second
        written[n, 2] = new_master
        weights_out[n] = new_master.astype(jnp.bfloat16)
        for i, target in enumerate(targets):
            result = weights_out.at[n] if i == 3 else written.at[n, i]
            copy = pltpu.make_async_copy(result, target.at[:, at], out_sems.at[n, i])
            copy.start()
            stores.append(copy)
    for copy in stores:
        copy.wait()


def adam(place, slots, shared, pairs, moment, second, master):
    own, rows = moment.shape
    piece = rows // 8
    hbm = pl.BlockSpec(memory_space=pltpu.HBM)
    wide = jax.ShapeDtypeStruct((own, rows), jnp.float32)
    flat = [a for pair in pairs for a in pair] + [moment, second, master]
    flat = [pltpu.with_memory_space_constraint(a, pltpu.HBM) for a in flat]
    return pl.pallas_call(
        functools.partial(adam_kernel, slots),
        in_specs=[SCALARS, WHOLE] + [hbm] * len(flat),
        out_specs=[hbm] * 4,
        scratch_shapes=[
            pltpu.VMEM((8, own, piece), jnp.bfloat16),
            pltpu.VMEM((8, 3, own, piece), jnp.float32),
            pltpu.VMEM((8, 3, own, piece), jnp.float32),
            pltpu.VMEM((8, own, piece), jnp.bfloat16),
            pltpu.SemaphoreType.DMA((8, 4)),
            pltpu.SemaphoreType.DMA((8, 4)),
        ],
        out_shape=[wide, wide, wide, jax.ShapeDtypeStruct((own, rows), jnp.bfloat16)],
        compiler_params=pltpu.CompilerParams(vmem_limit_bytes=60 * 2**20),
        cost_estimate=pl.CostEstimate(flops=10**7, bytes_accessed=17 * 10**6, transcendentals=10**6),
        name="adam",
    )(place, shared, *flat)


PRODUCTS = ((0,), (3, 1), (2,))
EARLY = 2


def step(activations, out_grads, act_scale, grad_scale, moment, second, master):
    place = jnp.stack([lax.axis_index(a).astype(jnp.int32) for a in ("z", "x", "c", "y")])
    piece = activations.shape[2] // 8

    mine, theirs = slab(place, activations, act_scale)
    held_own = jnp.concatenate([mine, swapped(theirs)], 0)
    near = [gathered(held_own, k) for k in (1, 2, 3)]

    lefts = prep_grads(place, out_grads, swapped(out_grads), grad_scale, swapped(grad_scale))
    lefts = [lefts[0]] + [gathered(lefts[k], k) for k in (1, 2, 3)]

    acts, opposite = all_acts(place, activations, swapped(activations), act_scale, swapped(act_scale))

    held = jnp.stack(near)
    across = [gathered(opposite, k) for k in (1, 2, 3)]
    sources = {0: held, 3: along_y(held, 1), 1: along_y(held, 3)}
    rights = {offset: [(array, lead) for lead in range(3)] for offset, array in sources.items()}
    rights[2] = [(array, None) for array in across]

    pieces, slots = [], []
    for number, offsets in enumerate(PRODUCTS):
        slots += [(offset, number, n) for n, offset in enumerate(offsets)]
        parts = product(place, offsets, lefts, acts, [rights[offset] for offset in offsets], piece)
        pieces.append([parts[0]] + [scattered(parts[k], k) for k in (1, 2, 3)])

    kept, given, squares = sums(place, pieces[:EARLY])
    more_kept, more_given, squares = sums(place, pieces[EARLY:], squares)
    kept, given = kept + more_kept, given + more_given
    pairs = [(own, swapped(other)) for own, other in zip(kept, given)]
    shared = lax.all_to_all(squares, ALL, 0, 0, tiled=True)
    return tuple(adam(place, slots, shared, pairs, moment, second, master))


def solution(mesh):
    finer = Mesh(mesh.devices.reshape(4, 4, 2, mesh.shape["tensor"]), ALL)
    in_specs = (
        P(DP, None, None),
        P(DP, None, "y"),
        P(DP, None),
        P(DP, None, "y"),
        P(TENSOR_DP, None),
        P(TENSOR_DP, None),
        P(TENSOR_DP, None),
    )
    out_specs = (P(TENSOR_DP, None),) * 4
    return jax.shard_map(step, mesh=finer, in_specs=in_specs, out_specs=out_specs, check_vma=False)
```

```python
import functools

import jax
import jax.numpy as jnp
from jax import lax
from jax.experimental import pallas as pl
from jax.experimental.pallas import tpu as pltpu
from jax.sharding import Mesh
from jax.sharding import PartitionSpec as P


FF = 20480
ROWS = 4096
TILE = 128
DP = ("z", "x", "c")
ALL = ("z", "x", "c", "y")
TENSOR_DP = ("y", "z", "x", "c")


clip_rms = 1.0
beta_first = 0.9
beta_second = 0.95
learn_rate = 0.003
adam_eps = 1e-08

SWAP = [(0, 1), (1, 0)]
WHOLE = pl.BlockSpec(memory_space=pltpu.VMEM)
SCALARS = pl.BlockSpec(memory_space=pltpu.SMEM)


def ring(shift):
    return [(i, (i + shift) % 4) for i in range(4)]


def crossed(shift, first_over_z):
    pairs = []
    for z in range(4):
        for x in range(4):
            for c in range(2):
                over_z = (c == 0) == first_over_z
                to = ((z + shift) % 4, x) if over_z else (z, (x + shift) % 4)
                pairs.append(((z * 4 + x) * 2 + c, (to[0] * 4 + to[1]) * 2 + c))
    return pairs


def gathered(a, k):
    return lax.ppermute(a, DP, crossed(k, True))


def scattered(a, k):
    return lax.ppermute(a, DP, crossed(k, False))


def along_y(a, k):
    return lax.ppermute(a, "y", ring(k))


def swapped(a):
    return lax.ppermute(a, "c", SWAP)


def gather_at(place_ref):
    return jnp.where(place_ref[2] == 0, place_ref[0], place_ref[1])


def reduce_at(place_ref):
    return jnp.where(place_ref[2] == 0, place_ref[1], place_ref[0])


def dequantized(acts_ref, scale_ref, at):
    blocks, tile, width = acts_ref.shape
    scales = scale_ref[...].astype(jnp.float32)
    lane = lax.broadcasted_iota(jnp.int32, scales.shape, 1)
    strips = []
    for t in range(width // TILE):
        chosen = jnp.sum(jnp.where(lane == at * (width // TILE) + t, scales, 0.0), axis=1, keepdims=True)
        strip = acts_ref[:, :, t * TILE : (t + 1) * TILE].astype(jnp.float32) * chosen[:, :, None]
        strips.append(strip.astype(jnp.bfloat16).reshape(blocks * tile, TILE))
    return strips


def slab_kernel(place_ref, mine_ref, theirs_ref, scale_ref, *outs):
    core, y = place_ref[2], place_ref[3]
    for source, at, out in ((mine_ref, 2 * y + core, outs[0]), (theirs_ref, 2 * y + 1 - core, outs[1])):
        for t, strip in enumerate(dequantized(source, scale_ref, at)):
            out[:, t * TILE : (t + 1) * TILE] = strip


def slab(place, activations, act_scale):
    blocks, tile, rows = activations.shape
    piece = rows // 8
    shape = jax.ShapeDtypeStruct((blocks * tile, piece), jnp.bfloat16)
    acts = pltpu.with_memory_space_constraint(activations, pltpu.HBM)
    return pl.pallas_call(
        slab_kernel,
        grid_spec=pltpu.PrefetchScalarGridSpec(
            num_scalar_prefetch=1,
            grid=(1,),
            in_specs=[
                pl.BlockSpec((blocks, tile, piece), lambda j, p: (0, 0, 2 * p[3] + p[2])),
                pl.BlockSpec((blocks, tile, piece), lambda j, p: (0, 0, 2 * p[3] + 1 - p[2])),
                pl.BlockSpec(act_scale.shape, lambda j, p: (0, 0)),
            ],
            out_specs=[pl.BlockSpec(shape.shape, lambda j, p: (0, 0))] * 2,
        ),
        out_shape=[shape, shape],
        compiler_params=pltpu.CompilerParams(vmem_limit_bytes=8 * 2**20),
        cost_estimate=pl.CostEstimate(flops=10**6, bytes_accessed=10**6, transcendentals=0),
        name="slab",
    )(place, acts, acts, pltpu.with_memory_space_constraint(act_scale, pltpu.HBM))


def acts_kernel(place_ref, own_ref, other_ref, own_scale_ref, other_scale_ref, whole_ref, opposite_ref):
    j = pl.program_id(0)
    tokens = whole_ref.shape[0] // 2
    at = 2 * j + place_ref[2]
    for n, (source, scale) in enumerate(((own_ref, own_scale_ref), (other_ref, other_scale_ref))):
        for t, strip in enumerate(dequantized(source, scale, at)):
            whole_ref[n * tokens : (n + 1) * tokens, t * TILE : (t + 1) * TILE] = strip

    @pl.when(lax.rem(place_ref[3] + 2, 4) == j)
    def _():
        opposite_ref[...] = whole_ref[...]


def all_acts(place, own, other, own_scale, other_scale):
    blocks, tile, rows = own.shape
    tokens, piece = 2 * blocks * tile, rows // 8
    block = pl.BlockSpec((blocks, tile, piece), lambda j, p: (0, 0, 2 * j + p[2]))
    scale = pl.BlockSpec(own_scale.shape, lambda j, p: (0, 0))
    return pl.pallas_call(
        acts_kernel,
        grid_spec=pltpu.PrefetchScalarGridSpec(
            num_scalar_prefetch=1,
            grid=(4,),
            in_specs=[block, block, scale, scale],
            out_specs=[
                pl.BlockSpec((tokens, piece), lambda j, p: (0, j)),
                pl.BlockSpec((tokens, piece), lambda j, p: (0, 0)),
            ],
        ),
        out_shape=[
            jax.ShapeDtypeStruct((tokens, 4 * piece), jnp.bfloat16),
            jax.ShapeDtypeStruct((tokens, piece), jnp.bfloat16),
        ],
        compiler_params=pltpu.CompilerParams(vmem_limit_bytes=8 * 2**20),
        cost_estimate=pl.CostEstimate(flops=10**6, bytes_accessed=4 * 10**6, transcendentals=0),
        name="acts",
    )(place, pltpu.with_memory_space_constraint(own, pltpu.HBM), other, own_scale, other_scale)


def prep_kernel(place_ref, own_ref, other_ref, own_scale_ref, other_scale_ref, *refs):
    outs, turned = refs[:4], refs[4]
    tokens = own_ref.shape[0] * own_ref.shape[1]
    columns = own_ref.shape[2]
    for n, (source, scale) in enumerate(((own_ref, own_scale_ref), (other_ref, other_scale_ref))):
        deq = (source[...].astype(jnp.float32) * scale[...].astype(jnp.float32)).reshape(tokens, columns)
        turned[:, n * tokens : (n + 1) * tokens] = deq.T.astype(jnp.bfloat16)
    both = columns // 4
    j = pl.program_id(0)
    me = gather_at(place_ref)
    for k in range(4):
        to = lax.rem(me + k, 4)

        @pl.when(jnp.logical_and(place_ref[2] == 0, to == j))
        def _(k=k):
            outs[k][...] = turned[...]

        @pl.when(place_ref[2] == 1)
        def _(k=k, to=to):
            at = pl.multiple_of(to * both, 32)
            outs[k][pl.ds(pl.multiple_of(j * both, 32), both), :] = turned[pl.ds(at, both), :]


def prep_grads(place, own, other, own_scale, other_scale):
    blocks, tile, columns = own.shape
    tokens = blocks * tile
    part = columns // 4
    shape = jax.ShapeDtypeStruct((part, 2 * tokens), jnp.bfloat16)
    block = pl.BlockSpec((blocks, tile, part), lambda j, p: (0, 0, j))
    scale = pl.BlockSpec((blocks, 1, part), lambda j, p: (0, 0, j))
    return pl.pallas_call(
        prep_kernel,
        grid_spec=pltpu.PrefetchScalarGridSpec(
            num_scalar_prefetch=1,
            grid=(4,),
            in_specs=[block, block, scale, scale],
            out_specs=[pl.BlockSpec(shape.shape, lambda j, p: (0, 0))] * 4,
            scratch_shapes=[pltpu.VMEM(shape.shape, jnp.bfloat16)],
        ),
        out_shape=[shape] * 4,
        compiler_params=pltpu.CompilerParams(vmem_limit_bytes=20 * 2**20),
        cost_estimate=pl.CostEstimate(flops=10**9, bytes_accessed=8 * columns * tokens, transcendentals=0),
        name="prep",
    )(place, pltpu.with_memory_space_constraint(own, pltpu.HBM), other, own_scale, other_scale)


def product_kernel(offsets, forms, width, place_ref, *refs):
    lefts, refs = refs[:4], refs[4:]
    outs, total = refs[-5:-1], refs[-1]
    me = reduce_at(place_ref)
    columns = total.shape[0]
    both = columns // 4
    for group, form in enumerate(forms):
        at = pl.multiple_of(lax.rem(place_ref[3] + offsets[group], 4) * width, width)
        for start in range(0, columns, columns // 2):
            value = None
            for left, (which, lead) in zip(lefts, form):
                if which == 0:
                    cols = refs[0][:, pl.ds(at, width)]
                else:
                    cols = refs[which][...] if lead is None else refs[which][lead]
                term = jnp.dot(left[start : start + columns // 2, :], cols, preferred_element_type=jnp.float32)
                value = term if value is None else value + term
            total[start : start + columns // 2, :] = value
        for k in range(4):
            row = pl.multiple_of(lax.rem(me + k, 4) * both, 32)
            outs[k][:, group * width : (group + 1) * width] = total[pl.ds(row, both), :].astype(jnp.bfloat16)


def product(place, offsets, lefts, acts, groups, width):
    arrays, forms = [acts], []
    for rights in groups:
        form = [(0, None)]
        for array, lead in rights:
            known = [i for i, a in enumerate(arrays) if a is array]
            if not known:
                arrays.append(array)
                known = [len(arrays) - 1]
            form.append((known[0], lead))
        forms.append(form)
    columns, tokens = lefts[0].shape
    both = columns // 4
    return pl.pallas_call(
        functools.partial(product_kernel, offsets, forms, width),
        in_specs=[SCALARS] + [WHOLE] * (4 + len(arrays)),
        out_specs=[WHOLE] * 4,
        scratch_shapes=[pltpu.VMEM((columns, width), jnp.float32)],
        out_shape=[jax.ShapeDtypeStruct((both, width * len(groups)), jnp.bfloat16)] * 4,
        compiler_params=pltpu.CompilerParams(vmem_limit_bytes=12 * 2**20),
        cost_estimate=pl.CostEstimate(
            flops=8 * columns * tokens * width * len(groups),
            bytes_accessed=8 * tokens * (columns + width),
            transcendentals=0,
        ),
        name="product",
    )(place, *lefts, *arrays)


def folded(squares):
    high, wide = squares.shape
    value = None
    for r in range(0, high, 8):
        for w in range(0, wide, 128):
            term = squares[r : r + 8, w : w + 128]
            value = term if value is None else value + term
    return value


def sums_kernel(count, last, place_ref, *refs):
    parts, refs = refs[: 4 * count], refs[4 * count :]
    before, refs = (refs[0], refs[1:]) if last else (None, refs)
    squares = before[...] if last else None
    own = refs[0].shape[0]
    core = place_ref[2]
    for n in range(count):
        for side in range(2):
            who = core if side == 0 else 1 - core
            at = pl.ds(pl.multiple_of(who * own, 32), own)
            value = parts[4 * n][at, :].astype(jnp.float32)
            for k in range(1, 4):
                value = value + parts[4 * n + k][at, :].astype(jnp.float32)
            refs[2 * n + side][...] = value.astype(jnp.bfloat16)
            term = folded(value * value)
            squares = term if squares is None else squares + term
    if last:
        refs[-1][...] = jnp.broadcast_to(jnp.sum(squares, keepdims=True)[None], refs[-1].shape)
    else:
        refs[-1][...] = squares


def sums(place, pieces, before=None):
    last = before is not None
    flat = [p for piece in pieces for p in piece] + ([before] if last else [])
    shapes = []
    for piece in pieces:
        both, width = piece[0].shape
        shapes += [pltpu.HBM((both // 2, width), jnp.bfloat16)] * 2
    shapes.append(jax.ShapeDtypeStruct((128, 1, 128) if last else (8, 128), jnp.float32))
    *values, squares = pl.pallas_call(
        functools.partial(sums_kernel, len(pieces), last),
        in_specs=[SCALARS] + [WHOLE] * len(flat),
        out_specs=[WHOLE] * len(shapes),
        out_shape=shapes,
        compiler_params=pltpu.CompilerParams(vmem_limit_bytes=8 * 2**20),
        cost_estimate=pl.CostEstimate(flops=10**8, bytes_accessed=4 * 10**6, transcendentals=0),
        name="sums",
    )(place, *flat)
    return values[::2], values[1::2], squares


def adam_kernel(slots, place_ref, shared, *refs):
    count = 2 * len({which for _, which, _ in slots})
    grads, refs = refs[:count], refs[count:]
    sources, held, targets = refs[:2], refs[2], refs[3:7]
    grad_in, read, written, weights_out, in_sems, out_sems = refs[7:]
    piece = grad_in.shape[2]
    core, y = place_ref[2], place_ref[3]
    blocks = [(offset, which, lead, side) for offset, which, lead in slots for side in range(2)]
    ats, fetches = [], []
    for n, (offset, which, lead, side) in enumerate(blocks):
        half = core if side == 0 else 1 - core
        at = pl.ds(pl.multiple_of((2 * lax.rem(y + offset, 4) + half) * piece, piece), piece)
        ats.append(at)
        from_grad = grads[2 * which + side].at[:, lead * piece : (lead + 1) * piece]
        copies = [pltpu.make_async_copy(from_grad, grad_in.at[n], in_sems.at[n, 3])]
        for i, source in enumerate(sources):
            copies.append(pltpu.make_async_copy(source.at[:, at], read.at[n, i], in_sems.at[n, i]))
        for copy in copies:
            copy.start()
        fetches.append(copies)

    norm = jnp.sqrt(jnp.sum(shared[...], axis=0))
    factor = jnp.minimum(1.0, clip_rms * jnp.sqrt(jnp.float32(FF * ROWS)) / norm)
    stores = []
    for n, at in enumerate(ats):
        for copy in fetches[n]:
            copy.wait()
        clipped = factor[0:1, 0:1] * grad_in[n].astype(jnp.float32)
        new_moment = beta_first * held[:, at] + (1.0 - beta_first) * clipped
        new_second = beta_second * read[n, 0] + (1.0 - beta_second) * clipped * clipped
        new_master = read[n, 1] - learn_rate * new_moment / (jnp.sqrt(new_second) + adam_eps)
        written[n, 0] = new_moment
        written[n, 1] = new_second
        written[n, 2] = new_master
        weights_out[n] = new_master.astype(jnp.bfloat16)
        for i, target in enumerate(targets):
            result = weights_out.at[n] if i == 3 else written.at[n, i]
            copy = pltpu.make_async_copy(result, target.at[:, at], out_sems.at[n, i])
            copy.start()
            stores.append(copy)
    for copy in stores:
        copy.wait()


def adam(place, slots, shared, pairs, moment, second, master):
    own, rows = moment.shape
    piece = rows // 8
    hbm = pl.BlockSpec(memory_space=pltpu.HBM)
    wide = jax.ShapeDtypeStruct((own, rows), jnp.float32)
    flat = [a for pair in pairs for a in pair] + [second, master]
    flat = [pltpu.with_memory_space_constraint(a, pltpu.HBM) for a in flat]
    moment = pltpu.with_memory_space_constraint(moment, pltpu.VMEM)
    return pl.pallas_call(
        functools.partial(adam_kernel, slots),
        in_specs=[SCALARS, WHOLE] + [hbm] * len(flat) + [WHOLE],
        out_specs=[hbm] * 4,
        scratch_shapes=[
            pltpu.VMEM((8, own, piece), jnp.bfloat16),
            pltpu.VMEM((8, 2, own, piece), jnp.float32),
            pltpu.VMEM((8, 3, own, piece), jnp.float32),
            pltpu.VMEM((8, own, piece), jnp.bfloat16),
            pltpu.SemaphoreType.DMA((8, 4)),
            pltpu.SemaphoreType.DMA((8, 4)),
        ],
        out_shape=[wide, wide, wide, jax.ShapeDtypeStruct((own, rows), jnp.bfloat16)],
        compiler_params=pltpu.CompilerParams(vmem_limit_bytes=24 * 2**20),
        cost_estimate=pl.CostEstimate(flops=10**7, bytes_accessed=17 * 10**6, transcendentals=10**6),
        name="adam",
    )(place, shared, *flat, moment)


PRODUCTS = ((0,), (3, 1), (2,))
EARLY = 2


def step(activations, out_grads, act_scale, grad_scale, moment, second, master):
    place = jnp.stack([lax.axis_index(a).astype(jnp.int32) for a in ("z", "x", "c", "y")])
    piece = activations.shape[2] // 8

    mine, theirs = slab(place, activations, act_scale)
    held_own = jnp.concatenate([mine, swapped(theirs)], 0)
    near = [gathered(held_own, k) for k in (1, 2, 3)]

    lefts = prep_grads(place, out_grads, swapped(out_grads), grad_scale, swapped(grad_scale))
    lefts = [lefts[0]] + [gathered(lefts[k], k) for k in (1, 2, 3)]

    acts, opposite = all_acts(place, activations, swapped(activations), act_scale, swapped(act_scale))

    held = jnp.stack(near)
    across = [gathered(opposite, k) for k in (1, 2, 3)]
    sources = {0: held, 3: along_y(held, 1), 1: along_y(held, 3)}
    rights = {offset: [(array, lead) for lead in range(3)] for offset, array in sources.items()}
    rights[2] = [(array, None) for array in across]

    pieces, slots = [], []
    for number, offsets in enumerate(PRODUCTS):
        slots += [(offset, number, n) for n, offset in enumerate(offsets)]
        parts = product(place, offsets, lefts, acts, [rights[offset] for offset in offsets], piece)
        pieces.append([parts[0]] + [scattered(parts[k], k) for k in (1, 2, 3)])

    kept, given, squares = sums(place, pieces[:EARLY])
    more_kept, more_given, squares = sums(place, pieces[EARLY:], squares)
    kept, given = kept + more_kept, given + more_given
    pairs = [(own, swapped(other)) for own, other in zip(kept, given)]
    shared = lax.all_to_all(squares, ALL, 0, 0, tiled=True)
    return tuple(adam(place, slots, shared, pairs, moment, second, master))


def solution(mesh):
    finer = Mesh(mesh.devices.reshape(4, 4, 2, mesh.shape["tensor"]), ALL)
    in_specs = (
        P(DP, None, None),
        P(DP, None, "y"),
        P(DP, None),
        P(DP, None, "y"),
        P(TENSOR_DP, None),
        P(TENSOR_DP, None),
        P(TENSOR_DP, None),
    )
    out_specs = (P(TENSOR_DP, None),) * 4
    return jax.shard_map(step, mesh=finer, in_specs=in_specs, out_specs=out_specs, check_vma=False)
```

```python
import functools

import jax
import jax.numpy as jnp
from jax import lax
from jax.experimental import pallas as pl
from jax.experimental.pallas import tpu as pltpu
from jax.sharding import Mesh
from jax.sharding import PartitionSpec as P


FF = 20480
ROWS = 4096
TILE = 128
DP = ("z", "x", "c")
ALL = ("z", "x", "c", "y")
TENSOR_DP = ("y", "z", "x", "c")


clip_rms = 1.0
beta_first = 0.9
beta_second = 0.95
learn_rate = 0.003
adam_eps = 1e-08

SWAP = [(0, 1), (1, 0)]
WHOLE = pl.BlockSpec(memory_space=pltpu.VMEM)
SCALARS = pl.BlockSpec(memory_space=pltpu.SMEM)


def ring(shift):
    return [(i, (i + shift) % 4) for i in range(4)]


def crossed(shift, first_over_z):
    pairs = []
    for z in range(4):
        for x in range(4):
            for c in range(2):
                over_z = (c == 0) == first_over_z
                to = ((z + shift) % 4, x) if over_z else (z, (x + shift) % 4)
                pairs.append(((z * 4 + x) * 2 + c, (to[0] * 4 + to[1]) * 2 + c))
    return pairs


def gathered(a, k):
    return lax.ppermute(a, DP, crossed(k, True))


def scattered(a, k):
    return lax.ppermute(a, DP, crossed(k, False))


def along_y(a, k):
    return lax.ppermute(a, "y", ring(k))


def swapped(a):
    return lax.ppermute(a, "c", SWAP)


def gather_at(place_ref):
    return jnp.where(place_ref[2] == 0, place_ref[0], place_ref[1])


def reduce_at(place_ref):
    return jnp.where(place_ref[2] == 0, place_ref[1], place_ref[0])


def dequantized(acts_ref, scale_ref, at):
    blocks, tile, width = acts_ref.shape
    scales = scale_ref[...].astype(jnp.float32)
    lane = lax.broadcasted_iota(jnp.int32, scales.shape, 1)
    strips = []
    for t in range(width // TILE):
        chosen = jnp.sum(jnp.where(lane == at * (width // TILE) + t, scales, 0.0), axis=1, keepdims=True)
        strip = acts_ref[:, :, t * TILE : (t + 1) * TILE].astype(jnp.float32) * chosen[:, :, None]
        strips.append(strip.astype(jnp.bfloat16).reshape(blocks * tile, TILE))
    return strips


def slab_kernel(place_ref, mine_ref, theirs_ref, scale_ref, *outs):
    core, y = place_ref[2], place_ref[3]
    for source, at, out in ((mine_ref, 2 * y + core, outs[0]), (theirs_ref, 2 * y + 1 - core, outs[1])):
        for t, strip in enumerate(dequantized(source, scale_ref, at)):
            out[:, t * TILE : (t + 1) * TILE] = strip


def slab(place, activations, act_scale):
    blocks, tile, rows = activations.shape
    piece = rows // 8
    shape = jax.ShapeDtypeStruct((blocks * tile, piece), jnp.bfloat16)
    acts = pltpu.with_memory_space_constraint(activations, pltpu.HBM)
    return pl.pallas_call(
        slab_kernel,
        grid_spec=pltpu.PrefetchScalarGridSpec(
            num_scalar_prefetch=1,
            grid=(1,),
            in_specs=[
                pl.BlockSpec((blocks, tile, piece), lambda j, p: (0, 0, 2 * p[3] + p[2])),
                pl.BlockSpec((blocks, tile, piece), lambda j, p: (0, 0, 2 * p[3] + 1 - p[2])),
                pl.BlockSpec(act_scale.shape, lambda j, p: (0, 0)),
            ],
            out_specs=[pl.BlockSpec(shape.shape, lambda j, p: (0, 0))] * 2,
        ),
        out_shape=[shape, shape],
        compiler_params=pltpu.CompilerParams(vmem_limit_bytes=8 * 2**20),
        cost_estimate=pl.CostEstimate(flops=10**6, bytes_accessed=10**6, transcendentals=0),
        name="slab",
    )(place, acts, acts, pltpu.with_memory_space_constraint(act_scale, pltpu.HBM))


def acts_kernel(place_ref, own_ref, other_ref, own_scale_ref, other_scale_ref, whole_ref, opposite_ref):
    j = pl.program_id(0)
    tokens = whole_ref.shape[0] // 2
    at = 2 * j + place_ref[2]
    for n, (source, scale) in enumerate(((own_ref, own_scale_ref), (other_ref, other_scale_ref))):
        for t, strip in enumerate(dequantized(source, scale, at)):
            whole_ref[n * tokens : (n + 1) * tokens, t * TILE : (t + 1) * TILE] = strip

    @pl.when(lax.rem(place_ref[3] + 2, 4) == j)
    def _():
        opposite_ref[...] = whole_ref[...]


def all_acts(place, own, other, own_scale, other_scale):
    blocks, tile, rows = own.shape
    tokens, piece = 2 * blocks * tile, rows // 8
    block = pl.BlockSpec((blocks, tile, piece), lambda j, p: (0, 0, 2 * j + p[2]))
    scale = pl.BlockSpec(own_scale.shape, lambda j, p: (0, 0))
    return pl.pallas_call(
        acts_kernel,
        grid_spec=pltpu.PrefetchScalarGridSpec(
            num_scalar_prefetch=1,
            grid=(4,),
            in_specs=[block, block, scale, scale],
            out_specs=[
                pl.BlockSpec((tokens, piece), lambda j, p: (0, j)),
                pl.BlockSpec((tokens, piece), lambda j, p: (0, 0)),
            ],
        ),
        out_shape=[
            jax.ShapeDtypeStruct((tokens, 4 * piece), jnp.bfloat16),
            jax.ShapeDtypeStruct((tokens, piece), jnp.bfloat16),
        ],
        compiler_params=pltpu.CompilerParams(vmem_limit_bytes=8 * 2**20),
        cost_estimate=pl.CostEstimate(flops=10**6, bytes_accessed=4 * 10**6, transcendentals=0),
        name="acts",
    )(place, pltpu.with_memory_space_constraint(own, pltpu.HBM), other, own_scale, other_scale)


def prep_kernel(place_ref, own_ref, other_ref, own_scale_ref, other_scale_ref, *refs):
    outs, turned = refs[:4], refs[4]
    tokens = own_ref.shape[0] * own_ref.shape[1]
    columns = own_ref.shape[2]
    for n, (source, scale) in enumerate(((own_ref, own_scale_ref), (other_ref, other_scale_ref))):
        deq = (source[...].astype(jnp.float32) * scale[...].astype(jnp.float32)).reshape(tokens, columns)
        turned[:, n * tokens : (n + 1) * tokens] = deq.T.astype(jnp.bfloat16)
    both = columns // 4
    j = pl.program_id(0)
    me = gather_at(place_ref)
    for k in range(4):
        to = lax.rem(me + k, 4)

        @pl.when(jnp.logical_and(place_ref[2] == 0, to == j))
        def _(k=k):
            outs[k][...] = turned[...]

        @pl.when(place_ref[2] == 1)
        def _(k=k, to=to):
            at = pl.multiple_of(to * both, 32)
            outs[k][pl.ds(pl.multiple_of(j * both, 32), both), :] = turned[pl.ds(at, both), :]


def prep_grads(place, own, other, own_scale, other_scale):
    blocks, tile, columns = own.shape
    tokens = blocks * tile
    part = columns // 4
    shape = jax.ShapeDtypeStruct((part, 2 * tokens), jnp.bfloat16)
    block = pl.BlockSpec((blocks, tile, part), lambda j, p: (0, 0, j))
    scale = pl.BlockSpec((blocks, 1, part), lambda j, p: (0, 0, j))
    return pl.pallas_call(
        prep_kernel,
        grid_spec=pltpu.PrefetchScalarGridSpec(
            num_scalar_prefetch=1,
            grid=(4,),
            in_specs=[block, block, scale, scale],
            out_specs=[pl.BlockSpec(shape.shape, lambda j, p: (0, 0))] * 4,
            scratch_shapes=[pltpu.VMEM(shape.shape, jnp.bfloat16)],
        ),
        out_shape=[shape] * 4,
        compiler_params=pltpu.CompilerParams(vmem_limit_bytes=20 * 2**20),
        cost_estimate=pl.CostEstimate(flops=10**9, bytes_accessed=8 * columns * tokens, transcendentals=0),
        name="prep",
    )(place, pltpu.with_memory_space_constraint(own, pltpu.HBM), other, own_scale, other_scale)


def product_kernel(offsets, forms, width, place_ref, *refs):
    lefts, refs = refs[:4], refs[4:]
    outs, total = refs[-5:-1], refs[-1]
    me = reduce_at(place_ref)
    columns = total.shape[0]
    both = columns // 4
    for group, form in enumerate(forms):
        at = pl.multiple_of(lax.rem(place_ref[3] + offsets[group], 4) * width, width)
        for start in range(0, columns, columns // 2):
            value = None
            for left, (which, lead) in zip(lefts, form):
                if which == 0:
                    cols = refs[0][:, pl.ds(at, width)]
                else:
                    cols = refs[which][...] if lead is None else refs[which][lead]
                term = jnp.dot(left[start : start + columns // 2, :], cols, preferred_element_type=jnp.float32)
                value = term if value is None else value + term
            total[start : start + columns // 2, :] = value
        for k in range(4):
            row = pl.multiple_of(lax.rem(me + k, 4) * both, 32)
            outs[k][:, group * width : (group + 1) * width] = total[pl.ds(row, both), :].astype(jnp.bfloat16)


def product(place, offsets, lefts, acts, groups, width):
    arrays, forms = [acts], []
    for rights in groups:
        form = [(0, None)]
        for array, lead in rights:
            known = [i for i, a in enumerate(arrays) if a is array]
            if not known:
                arrays.append(array)
                known = [len(arrays) - 1]
            form.append((known[0], lead))
        forms.append(form)
    columns, tokens = lefts[0].shape
    both = columns // 4
    return pl.pallas_call(
        functools.partial(product_kernel, offsets, forms, width),
        in_specs=[SCALARS] + [WHOLE] * (4 + len(arrays)),
        out_specs=[WHOLE] * 4,
        scratch_shapes=[pltpu.VMEM((columns, width), jnp.float32)],
        out_shape=[jax.ShapeDtypeStruct((both, width * len(groups)), jnp.bfloat16)] * 4,
        compiler_params=pltpu.CompilerParams(vmem_limit_bytes=12 * 2**20),
        cost_estimate=pl.CostEstimate(
            flops=8 * columns * tokens * width * len(groups),
            bytes_accessed=8 * tokens * (columns + width),
            transcendentals=0,
        ),
        name="product",
    )(place, *lefts, *arrays)


def folded(squares):
    high, wide = squares.shape
    value = None
    for r in range(0, high, 8):
        for w in range(0, wide, 128):
            term = squares[r : r + 8, w : w + 128]
            value = term if value is None else value + term
    return value


def sums_kernel(count, last, place_ref, *refs):
    parts, refs = refs[: 4 * count], refs[4 * count :]
    before, refs = (refs[0], refs[1:]) if last else (None, refs)
    squares = before[...] if last else None
    own = refs[0].shape[0]
    core = place_ref[2]
    for n in range(count):
        for side in range(2):
            who = core if side == 0 else 1 - core
            at = pl.ds(pl.multiple_of(who * own, 32), own)
            value = parts[4 * n][at, :].astype(jnp.float32)
            for k in range(1, 4):
                value = value + parts[4 * n + k][at, :].astype(jnp.float32)
            refs[2 * n + side][...] = value.astype(jnp.bfloat16)
            term = folded(value * value)
            squares = term if squares is None else squares + term
    if last:
        refs[-1][...] = jnp.broadcast_to(jnp.sum(squares, keepdims=True)[None], refs[-1].shape)
    else:
        refs[-1][...] = squares


def sums(place, pieces, before=None):
    last = before is not None
    flat = [p for piece in pieces for p in piece] + ([before] if last else [])
    shapes = []
    for piece in pieces:
        both, width = piece[0].shape
        shapes += [pltpu.HBM((both // 2, width), jnp.bfloat16)] * 2
    shapes.append(jax.ShapeDtypeStruct((128, 1, 128) if last else (8, 128), jnp.float32))
    *values, squares = pl.pallas_call(
        functools.partial(sums_kernel, len(pieces), last),
        in_specs=[SCALARS] + [WHOLE] * len(flat),
        out_specs=[WHOLE] * len(shapes),
        out_shape=shapes,
        compiler_params=pltpu.CompilerParams(vmem_limit_bytes=8 * 2**20),
        cost_estimate=pl.CostEstimate(flops=10**8, bytes_accessed=4 * 10**6, transcendentals=0),
        name="sums",
    )(place, *flat)
    return values[::2], values[1::2], squares


def adam_kernel(slots, place_ref, shared, *refs):
    count = 2 * len({which for _, which, _ in slots})
    grads, refs = refs[:count], refs[count:]
    sources, held, targets = refs[:2], refs[2], refs[3:7]
    grad_in, read, written, weights_out, in_sems, out_sems = refs[7:]
    piece = grad_in.shape[2]
    core, y = place_ref[2], place_ref[3]
    blocks = [(offset, which, lead, side) for offset, which, lead in slots for side in range(2)]
    ats, fetches = [], []
    for n, (offset, which, lead, side) in enumerate(blocks):
        half = core if side == 0 else 1 - core
        at = pl.ds(pl.multiple_of((2 * lax.rem(y + offset, 4) + half) * piece, piece), piece)
        ats.append(at)
        copies = []
        if side == 0:
            from_grad = grads[2 * which].at[:, lead * piece : (lead + 1) * piece]
            copies.append(pltpu.make_async_copy(from_grad, grad_in.at[n // 2], in_sems.at[n, 3]))
        for i, source in enumerate(sources):
            copies.append(pltpu.make_async_copy(source.at[:, at], read.at[n, i], in_sems.at[n, i]))
        for copy in copies:
            copy.start()
        fetches.append(copies)

    norm = jnp.sqrt(jnp.sum(shared[...], axis=0))
    factor = jnp.minimum(1.0, clip_rms * jnp.sqrt(jnp.float32(FF * ROWS)) / norm)
    stores = []
    for n, at in enumerate(ats):
        for copy in fetches[n]:
            copy.wait()
        _, which, lead, side = blocks[n]
        grad = grad_in[n // 2] if side == 0 else grads[2 * which + 1][:, lead * piece : (lead + 1) * piece]
        clipped = factor[0:1, 0:1] * grad.astype(jnp.float32)
        new_moment = beta_first * held[:, at] + (1.0 - beta_first) * clipped
        new_second = beta_second * read[n, 0] + (1.0 - beta_second) * clipped * clipped
        new_master = read[n, 1] - learn_rate * new_moment / (jnp.sqrt(new_second) + adam_eps)
        written[n, 0] = new_moment
        written[n, 1] = new_second
        written[n, 2] = new_master
        weights_out[n] = new_master.astype(jnp.bfloat16)
        for i, target in enumerate(targets):
            result = weights_out.at[n] if i == 3 else written.at[n, i]
            copy = pltpu.make_async_copy(result, target.at[:, at], out_sems.at[n, i])
            copy.start()
            stores.append(copy)
    for copy in stores:
        copy.wait()


def adam(place, slots, shared, pairs, moment, second, master):
    own, rows = moment.shape
    piece = rows // 8
    hbm = pl.BlockSpec(memory_space=pltpu.HBM)
    wide = jax.ShapeDtypeStruct((own, rows), jnp.float32)
    flat = [a for pair in pairs for a in pair] + [second, master, moment]
    spaces = [pltpu.HBM, pltpu.VMEM] * len(pairs) + [pltpu.HBM, pltpu.HBM, pltpu.VMEM]
    flat = [pltpu.with_memory_space_constraint(a, space) for a, space in zip(flat, spaces)]
    return pl.pallas_call(
        functools.partial(adam_kernel, slots),
        in_specs=[SCALARS, WHOLE] + [pl.BlockSpec(memory_space=space) for space in spaces],
        out_specs=[hbm] * 4,
        scratch_shapes=[
            pltpu.VMEM((4, own, piece), jnp.bfloat16),
            pltpu.VMEM((8, 2, own, piece), jnp.float32),
            pltpu.VMEM((8, 3, own, piece), jnp.float32),
            pltpu.VMEM((8, own, piece), jnp.bfloat16),
            pltpu.SemaphoreType.DMA((8, 4)),
            pltpu.SemaphoreType.DMA((8, 4)),
        ],
        out_shape=[wide, wide, wide, jax.ShapeDtypeStruct((own, rows), jnp.bfloat16)],
        compiler_params=pltpu.CompilerParams(vmem_limit_bytes=24 * 2**20),
        cost_estimate=pl.CostEstimate(flops=10**7, bytes_accessed=17 * 10**6, transcendentals=10**6),
        name="adam",
    )(place, shared, *flat)


PRODUCTS = ((0,), (3, 1), (2,))
EARLY = 2


def step(activations, out_grads, act_scale, grad_scale, moment, second, master):
    place = jnp.stack([lax.axis_index(a).astype(jnp.int32) for a in ("z", "x", "c", "y")])
    piece = activations.shape[2] // 8

    mine, theirs = slab(place, activations, act_scale)
    held_own = jnp.concatenate([mine, swapped(theirs)], 0)
    near = [gathered(held_own, k) for k in (1, 2, 3)]

    lefts = prep_grads(place, out_grads, swapped(out_grads), grad_scale, swapped(grad_scale))
    lefts = [lefts[0]] + [gathered(lefts[k], k) for k in (1, 2, 3)]

    acts, opposite = all_acts(place, activations, swapped(activations), act_scale, swapped(act_scale))

    held = jnp.stack(near)
    across = [gathered(opposite, k) for k in (1, 2, 3)]
    sources = {0: held, 3: along_y(held, 1), 1: along_y(held, 3)}
    rights = {offset: [(array, lead) for lead in range(3)] for offset, array in sources.items()}
    rights[2] = [(array, None) for array in across]

    pieces, slots = [], []
    for number, offsets in enumerate(PRODUCTS):
        slots += [(offset, number, n) for n, offset in enumerate(offsets)]
        parts = product(place, offsets, lefts, acts, [rights[offset] for offset in offsets], piece)
        pieces.append([parts[0]] + [scattered(parts[k], k) for k in (1, 2, 3)])

    kept, given, squares = sums(place, pieces[:EARLY])
    more_kept, more_given, squares = sums(place, pieces[EARLY:], squares)
    kept, given = kept + more_kept, given + more_given
    pairs = [(own, swapped(other)) for own, other in zip(kept, given)]
    shared = lax.all_to_all(squares, ALL, 0, 0, tiled=True)
    return tuple(adam(place, slots, shared, pairs, moment, second, master))


def solution(mesh):
    finer = Mesh(mesh.devices.reshape(4, 4, 2, mesh.shape["tensor"]), ALL)
    in_specs = (
        P(DP, None, None),
        P(DP, None, "y"),
        P(DP, None),
        P(DP, None, "y"),
        P(TENSOR_DP, None),
        P(TENSOR_DP, None),
        P(TENSOR_DP, None),
    )
    out_specs = (P(TENSOR_DP, None),) * 4
    return jax.shard_map(step, mesh=finer, in_specs=in_specs, out_specs=out_specs, check_vma=False)
```

```python
import functools

import jax
import jax.numpy as jnp
from jax import lax
from jax.experimental import pallas as pl
from jax.experimental.pallas import tpu as pltpu
from jax.sharding import Mesh
from jax.sharding import PartitionSpec as P


FF = 20480
ROWS = 4096
TILE = 128
DP = ("z", "x", "c")
ALL = ("z", "x", "c", "y")
TENSOR_DP = ("y", "z", "x", "c")


clip_rms = 1.0
beta_first = 0.9
beta_second = 0.95
learn_rate = 0.003
adam_eps = 1e-08

SWAP = [(0, 1), (1, 0)]
WHOLE = pl.BlockSpec(memory_space=pltpu.VMEM)
SCALARS = pl.BlockSpec(memory_space=pltpu.SMEM)


def ring(shift):
    return [(i, (i + shift) % 4) for i in range(4)]


def crossed(shift, first_over_z):
    pairs = []
    for z in range(4):
        for x in range(4):
            for c in range(2):
                over_z = (c == 0) == first_over_z
                to = ((z + shift) % 4, x) if over_z else (z, (x + shift) % 4)
                pairs.append(((z * 4 + x) * 2 + c, (to[0] * 4 + to[1]) * 2 + c))
    return pairs


def gathered(a, k):
    return lax.ppermute(a, DP, crossed(k, True))


def scattered(a, k):
    return lax.ppermute(a, DP, crossed(k, False))


def along_y(a, k):
    return lax.ppermute(a, "y", ring(k))


def swapped(a):
    return lax.ppermute(a, "c", SWAP)


def gather_at(place_ref):
    return jnp.where(place_ref[2] == 0, place_ref[0], place_ref[1])


def reduce_at(place_ref):
    return jnp.where(place_ref[2] == 0, place_ref[1], place_ref[0])


def dequantized(acts_ref, scale_ref, at):
    blocks, tile, width = acts_ref.shape
    scales = scale_ref[...].astype(jnp.float32)
    lane = lax.broadcasted_iota(jnp.int32, scales.shape, 1)
    strips = []
    for t in range(width // TILE):
        chosen = jnp.sum(jnp.where(lane == at * (width // TILE) + t, scales, 0.0), axis=1, keepdims=True)
        strip = acts_ref[:, :, t * TILE : (t + 1) * TILE].astype(jnp.float32) * chosen[:, :, None]
        strips.append(strip.astype(jnp.bfloat16).reshape(blocks * tile, TILE))
    return strips


def slab_kernel(place_ref, mine_ref, theirs_ref, scale_ref, *outs):
    core, y = place_ref[2], place_ref[3]
    for source, at, out in ((mine_ref, 2 * y + core, outs[0]), (theirs_ref, 2 * y + 1 - core, outs[1])):
        for t, strip in enumerate(dequantized(source, scale_ref, at)):
            out[:, t * TILE : (t + 1) * TILE] = strip


def slab(place, activations, act_scale):
    blocks, tile, rows = activations.shape
    piece = rows // 8
    shape = jax.ShapeDtypeStruct((blocks * tile, piece), jnp.bfloat16)
    acts = pltpu.with_memory_space_constraint(activations, pltpu.HBM)
    return pl.pallas_call(
        slab_kernel,
        grid_spec=pltpu.PrefetchScalarGridSpec(
            num_scalar_prefetch=1,
            grid=(1,),
            in_specs=[
                pl.BlockSpec((blocks, tile, piece), lambda j, p: (0, 0, 2 * p[3] + p[2])),
                pl.BlockSpec((blocks, tile, piece), lambda j, p: (0, 0, 2 * p[3] + 1 - p[2])),
                pl.BlockSpec(act_scale.shape, lambda j, p: (0, 0)),
            ],
            out_specs=[pl.BlockSpec(shape.shape, lambda j, p: (0, 0))] * 2,
        ),
        out_shape=[shape, shape],
        compiler_params=pltpu.CompilerParams(vmem_limit_bytes=8 * 2**20),
        cost_estimate=pl.CostEstimate(flops=10**6, bytes_accessed=10**6, transcendentals=0),
        name="slab",
    )(place, acts, acts, pltpu.with_memory_space_constraint(act_scale, pltpu.HBM))


def acts_kernel(place_ref, own_ref, other_ref, own_scale_ref, other_scale_ref, whole_ref, opposite_ref):
    j = pl.program_id(0)
    tokens = whole_ref.shape[0] // 2
    at = 2 * j + place_ref[2]
    for n, (source, scale) in enumerate(((own_ref, own_scale_ref), (other_ref, other_scale_ref))):
        for t, strip in enumerate(dequantized(source, scale, at)):
            whole_ref[n * tokens : (n + 1) * tokens, t * TILE : (t + 1) * TILE] = strip

    @pl.when(lax.rem(place_ref[3] + 2, 4) == j)
    def _():
        opposite_ref[...] = whole_ref[...]


def all_acts(place, own, other, own_scale, other_scale):
    blocks, tile, rows = own.shape
    tokens, piece = 2 * blocks * tile, rows // 8
    block = pl.BlockSpec((blocks, tile, piece), lambda j, p: (0, 0, 2 * j + p[2]))
    scale = pl.BlockSpec(own_scale.shape, lambda j, p: (0, 0))
    return pl.pallas_call(
        acts_kernel,
        grid_spec=pltpu.PrefetchScalarGridSpec(
            num_scalar_prefetch=1,
            grid=(4,),
            in_specs=[block, block, scale, scale],
            out_specs=[
                pl.BlockSpec((tokens, piece), lambda j, p: (0, j)),
                pl.BlockSpec((tokens, piece), lambda j, p: (0, 0)),
            ],
        ),
        out_shape=[
            jax.ShapeDtypeStruct((tokens, 4 * piece), jnp.bfloat16),
            jax.ShapeDtypeStruct((tokens, piece), jnp.bfloat16),
        ],
        compiler_params=pltpu.CompilerParams(vmem_limit_bytes=8 * 2**20),
        cost_estimate=pl.CostEstimate(flops=10**6, bytes_accessed=4 * 10**6, transcendentals=0),
        name="acts",
    )(place, pltpu.with_memory_space_constraint(own, pltpu.HBM), other, own_scale, other_scale)


def prep_kernel(place_ref, own_ref, other_ref, own_scale_ref, other_scale_ref, *refs):
    outs, turned = refs[:4], refs[4]
    tokens = own_ref.shape[0] * own_ref.shape[1]
    columns = own_ref.shape[2]
    for n, (source, scale) in enumerate(((own_ref, own_scale_ref), (other_ref, other_scale_ref))):
        deq = (source[...].astype(jnp.float32) * scale[...].astype(jnp.float32)).reshape(tokens, columns)
        turned[:, n * tokens : (n + 1) * tokens] = deq.T.astype(jnp.bfloat16)
    both = columns // 4
    j = pl.program_id(0)
    me = gather_at(place_ref)
    for k in range(4):
        to = lax.rem(me + k, 4)

        @pl.when(jnp.logical_and(place_ref[2] == 0, to == j))
        def _(k=k):
            outs[k][...] = turned[...]

        @pl.when(place_ref[2] == 1)
        def _(k=k, to=to):
            at = pl.multiple_of(to * both, 32)
            outs[k][pl.ds(pl.multiple_of(j * both, 32), both), :] = turned[pl.ds(at, both), :]


def prep_grads(place, own, other, own_scale, other_scale):
    blocks, tile, columns = own.shape
    tokens = blocks * tile
    part = columns // 4
    shape = jax.ShapeDtypeStruct((part, 2 * tokens), jnp.bfloat16)
    block = pl.BlockSpec((blocks, tile, part), lambda j, p: (0, 0, j))
    scale = pl.BlockSpec((blocks, 1, part), lambda j, p: (0, 0, j))
    return pl.pallas_call(
        prep_kernel,
        grid_spec=pltpu.PrefetchScalarGridSpec(
            num_scalar_prefetch=1,
            grid=(4,),
            in_specs=[block, block, scale, scale],
            out_specs=[pl.BlockSpec(shape.shape, lambda j, p: (0, 0))] * 4,
            scratch_shapes=[pltpu.VMEM(shape.shape, jnp.bfloat16)],
        ),
        out_shape=[shape] * 4,
        compiler_params=pltpu.CompilerParams(vmem_limit_bytes=20 * 2**20),
        cost_estimate=pl.CostEstimate(flops=10**9, bytes_accessed=8 * columns * tokens, transcendentals=0),
        name="prep",
    )(place, pltpu.with_memory_space_constraint(own, pltpu.HBM), other, own_scale, other_scale)


def product_kernel(offsets, forms, width, place_ref, *refs):
    lefts, refs = refs[:4], refs[4:]
    outs, total = refs[-5:-1], refs[-1]
    me = reduce_at(place_ref)
    columns = total.shape[0]
    both = columns // 4
    for group, form in enumerate(forms):
        at = pl.multiple_of(lax.rem(place_ref[3] + offsets[group], 4) * width, width)
        for start in range(0, columns, columns // 2):
            value = None
            for left, (which, lead) in zip(lefts, form):
                if which == 0:
                    cols = refs[0][:, pl.ds(at, width)]
                else:
                    cols = refs[which][...] if lead is None else refs[which][lead]
                term = jnp.dot(left[start : start + columns // 2, :], cols, preferred_element_type=jnp.float32)
                value = term if value is None else value + term
            total[start : start + columns // 2, :] = value
        for k in range(4):
            row = pl.multiple_of(lax.rem(me + k, 4) * both, 32)
            outs[k][:, group * width : (group + 1) * width] = total[pl.ds(row, both), :].astype(jnp.bfloat16)


def product(place, offsets, lefts, acts, groups, width):
    arrays, forms = [acts], []
    for rights in groups:
        form = [(0, None)]
        for array, lead in rights:
            known = [i for i, a in enumerate(arrays) if a is array]
            if not known:
                arrays.append(array)
                known = [len(arrays) - 1]
            form.append((known[0], lead))
        forms.append(form)
    columns, tokens = lefts[0].shape
    both = columns // 4
    return pl.pallas_call(
        functools.partial(product_kernel, offsets, forms, width),
        in_specs=[SCALARS] + [WHOLE] * (4 + len(arrays)),
        out_specs=[WHOLE] * 4,
        scratch_shapes=[pltpu.VMEM((columns, width), jnp.float32)],
        out_shape=[jax.ShapeDtypeStruct((both, width * len(groups)), jnp.bfloat16)] * 4,
        compiler_params=pltpu.CompilerParams(vmem_limit_bytes=12 * 2**20),
        cost_estimate=pl.CostEstimate(
            flops=8 * columns * tokens * width * len(groups),
            bytes_accessed=8 * tokens * (columns + width),
            transcendentals=0,
        ),
        name="product",
    )(place, *lefts, *arrays)


def folded(squares):
    high, wide = squares.shape
    value = None
    for r in range(0, high, 8):
        for w in range(0, wide, 128):
            term = squares[r : r + 8, w : w + 128]
            value = term if value is None else value + term
    return value


def sums_kernel(count, last, place_ref, *refs):
    parts, refs = refs[: 4 * count], refs[4 * count :]
    before, refs = (refs[0], refs[1:]) if last else (None, refs)
    squares = before[...] if last else None
    own = refs[0].shape[0]
    core = place_ref[2]
    for n in range(count):
        for side in range(2):
            who = core if side == 0 else 1 - core
            at = pl.ds(pl.multiple_of(who * own, 32), own)
            value = parts[4 * n][at, :].astype(jnp.float32)
            for k in range(1, 4):
                value = value + parts[4 * n + k][at, :].astype(jnp.float32)
            refs[2 * n + side][...] = value.astype(jnp.bfloat16)
            term = folded(value * value)
            squares = term if squares is None else squares + term
    if last:
        refs[-1][...] = jnp.broadcast_to(jnp.sum(squares, keepdims=True)[None], refs[-1].shape)
    else:
        refs[-1][...] = squares


def sums(place, pieces, before=None):
    last = before is not None
    flat = [p for piece in pieces for p in piece] + ([before] if last else [])
    shapes = []
    for piece in pieces:
        both, width = piece[0].shape
        given = pltpu.HBM((both // 2, width), jnp.bfloat16)
        shapes += [jax.ShapeDtypeStruct((both // 2, width), jnp.bfloat16) if last else given, given]
    shapes.append(jax.ShapeDtypeStruct((128, 1, 128) if last else (8, 128), jnp.float32))
    *values, squares = pl.pallas_call(
        functools.partial(sums_kernel, len(pieces), last),
        in_specs=[SCALARS] + [WHOLE] * len(flat),
        out_specs=[WHOLE] * len(shapes),
        out_shape=shapes,
        compiler_params=pltpu.CompilerParams(vmem_limit_bytes=8 * 2**20),
        cost_estimate=pl.CostEstimate(flops=10**8, bytes_accessed=4 * 10**6, transcendentals=0),
        name="sums",
    )(place, *flat)
    return values[::2], values[1::2], squares


def adam_kernel(slots, place_ref, shared, *refs):
    count = 2 * len({which for _, which, _ in slots})
    grads, refs = refs[:count], refs[count:]
    sources, held, targets = refs[:2], refs[2], refs[3:7]
    grad_in, read, written, weights_out, in_sems, out_sems = refs[7:]
    piece = grad_in.shape[2]
    core, y = place_ref[2], place_ref[3]
    blocks = [(offset, which, lead, side) for offset, which, lead in slots for side in range(2)]
    ats, fetches = [], []
    for n, (offset, which, lead, side) in enumerate(blocks):
        half = core if side == 0 else 1 - core
        at = pl.ds(pl.multiple_of((2 * lax.rem(y + offset, 4) + half) * piece, piece), piece)
        ats.append(at)
        copies = []
        if side == 0 and which < EARLY:
            from_grad = grads[2 * which].at[:, lead * piece : (lead + 1) * piece]
            copies.append(pltpu.make_async_copy(from_grad, grad_in.at[n // 2], in_sems.at[n, 3]))
        for i, source in enumerate(sources):
            copies.append(pltpu.make_async_copy(source.at[:, at], read.at[n, i], in_sems.at[n, i]))
        for copy in copies:
            copy.start()
        fetches.append(copies)

    norm = jnp.sqrt(jnp.sum(shared[...], axis=0))
    factor = jnp.minimum(1.0, clip_rms * jnp.sqrt(jnp.float32(FF * ROWS)) / norm)
    stores = []
    for n, at in enumerate(ats):
        for copy in fetches[n]:
            copy.wait()
        _, which, lead, side = blocks[n]
        if side == 0 and which < EARLY:
            grad = grad_in[n // 2]
        else:
            grad = grads[2 * which + side][:, lead * piece : (lead + 1) * piece]
        clipped = factor[0:1, 0:1] * grad.astype(jnp.float32)
        new_moment = beta_first * held[:, at] + (1.0 - beta_first) * clipped
        new_second = beta_second * read[n, 0] + (1.0 - beta_second) * clipped * clipped
        new_master = read[n, 1] - learn_rate * new_moment / (jnp.sqrt(new_second) + adam_eps)
        written[n, 0] = new_moment
        written[n, 1] = new_second
        written[n, 2] = new_master
        weights_out[n] = new_master.astype(jnp.bfloat16)
        for i, target in enumerate(targets):
            result = weights_out.at[n] if i == 3 else written.at[n, i]
            copy = pltpu.make_async_copy(result, target.at[:, at], out_sems.at[n, i])
            copy.start()
            stores.append(copy)
    for copy in stores:
        copy.wait()


def adam(place, slots, shared, pairs, moment, second, master):
    own, rows = moment.shape
    piece = rows // 8
    hbm = pl.BlockSpec(memory_space=pltpu.HBM)
    wide = jax.ShapeDtypeStruct((own, rows), jnp.float32)
    flat = [a for pair in pairs for a in pair] + [second, master, moment]
    spaces = [pltpu.HBM, pltpu.VMEM] * EARLY + [pltpu.VMEM] * (2 * (len(pairs) - EARLY)) + [pltpu.HBM, pltpu.HBM, pltpu.VMEM]
    flat = [pltpu.with_memory_space_constraint(a, space) for a, space in zip(flat, spaces)]
    return pl.pallas_call(
        functools.partial(adam_kernel, slots),
        in_specs=[SCALARS, WHOLE] + [pl.BlockSpec(memory_space=space) for space in spaces],
        out_specs=[hbm] * 4,
        scratch_shapes=[
            pltpu.VMEM((4, own, piece), jnp.bfloat16),
            pltpu.VMEM((8, 2, own, piece), jnp.float32),
            pltpu.VMEM((8, 3, own, piece), jnp.float32),
            pltpu.VMEM((8, own, piece), jnp.bfloat16),
            pltpu.SemaphoreType.DMA((8, 4)),
            pltpu.SemaphoreType.DMA((8, 4)),
        ],
        out_shape=[wide, wide, wide, jax.ShapeDtypeStruct((own, rows), jnp.bfloat16)],
        compiler_params=pltpu.CompilerParams(vmem_limit_bytes=24 * 2**20),
        cost_estimate=pl.CostEstimate(flops=10**7, bytes_accessed=17 * 10**6, transcendentals=10**6),
        name="adam",
    )(place, shared, *flat)


PRODUCTS = ((0,), (3, 1), (2,))
EARLY = 2


def step(activations, out_grads, act_scale, grad_scale, moment, second, master):
    place = jnp.stack([lax.axis_index(a).astype(jnp.int32) for a in ("z", "x", "c", "y")])
    piece = activations.shape[2] // 8

    mine, theirs = slab(place, activations, act_scale)
    held_own = jnp.concatenate([mine, swapped(theirs)], 0)
    near = [gathered(held_own, k) for k in (1, 2, 3)]

    lefts = prep_grads(place, out_grads, swapped(out_grads), grad_scale, swapped(grad_scale))
    lefts = [lefts[0]] + [gathered(lefts[k], k) for k in (1, 2, 3)]

    acts, opposite = all_acts(place, activations, swapped(activations), act_scale, swapped(act_scale))

    held = jnp.stack(near)
    across = [gathered(opposite, k) for k in (1, 2, 3)]
    sources = {0: held, 3: along_y(held, 1), 1: along_y(held, 3)}
    rights = {offset: [(array, lead) for lead in range(3)] for offset, array in sources.items()}
    rights[2] = [(array, None) for array in across]

    pieces, slots = [], []
    for number, offsets in enumerate(PRODUCTS):
        slots += [(offset, number, n) for n, offset in enumerate(offsets)]
        parts = product(place, offsets, lefts, acts, [rights[offset] for offset in offsets], piece)
        pieces.append([parts[0]] + [scattered(parts[k], k) for k in (1, 2, 3)])

    kept, given, squares = sums(place, pieces[:EARLY])
    more_kept, more_given, squares = sums(place, pieces[EARLY:], squares)
    kept, given = kept + more_kept, given + more_given
    pairs = [(own, swapped(other)) for own, other in zip(kept, given)]
    shared = lax.all_to_all(squares, ALL, 0, 0, tiled=True)
    return tuple(adam(place, slots, shared, pairs, moment, second, master))


def solution(mesh):
    finer = Mesh(mesh.devices.reshape(4, 4, 2, mesh.shape["tensor"]), ALL)
    in_specs = (
        P(DP, None, None),
        P(DP, None, "y"),
        P(DP, None),
        P(DP, None, "y"),
        P(TENSOR_DP, None),
        P(TENSOR_DP, None),
        P(TENSOR_DP, None),
    )
    out_specs = (P(TENSOR_DP, None),) * 4
    return jax.shard_map(step, mesh=finer, in_specs=in_specs, out_specs=out_specs, check_vma=False)
```
